32 devices in a mesh: ep: 8 (over y, x, core), tp: 4 (over z).
Axes of the slice: x: 2, y: 2, z: 4, core: 2. Of those that a mesh axis runs over, the one named last changes fastest.
Arguments:
- tokens: bfloat16 [1024, 2048], P('ep', 'tp'), may hold values from -6 to 6
- routing: int32 [1024, 8], P('ep'), may hold values from 0 to 31, all different within a row; in each aligned block of 128 rows (0 to 127, 128 to 255, ...) at most 64 rows name the same one
- gate_fixed: int32 [1024, 8], P('ep'), may hold values from 1 to 65535
- gate_weight: bfloat16 [32, 2048, 768], P('ep', 'tp'), may hold values from -0.125 to 0.125
- up_weight: bfloat16 [32, 2048, 768], P('ep', 'tp'), may hold values from -0.1875 to 0.1875
- down_weight: bfloat16 [32, 2048, 768], P('ep', 'tp'), may hold values from -0.21875 to 0.21875
Outputs:
- layer_out: bfloat16 [1024, 2048], P('ep', 'tp')
The draws below stay inside these ranges and needn't reach their ends.
Inputs may be any that keep to these rules, and one draw needn't show every extreme that they name: `routing`: each token names 8 different experts. In each aligned block of 128 tokens (the tokens of one index of ep) no expert is named by more than 64 tokens, and in some blocks one expert is named by exactly 64.
All inputs are finite; a program needn't handle non-finite values.
Results may differ from the reference program's by a relative error of at most 0.0057.
Values may be sent and summed in bfloat16 or wider, within the bound.
A program may use at most 64 MiB of HBM per device.

```python
import math
import jax
import jax.numpy as jnp
import numpy as np
from jax import lax

D = 2048
FF = 768
TOP = 8
TOK_EP = 128
EXPERTS = 32
CAP = 64
TOKENS = 1024
N_EP = 8


def set_ends(result, stream_key, smallest, high):
    extent = result.shape
    place = [jax.random.randint(jax.random.fold_in(stream_key, axis), (), 0, extent[axis]) for axis in range(len(extent))]
    result = result.at[tuple(place)].set(smallest)
    longest = extent.index(max(extent))
    place[longest] = (place[longest] + 1) % extent[longest]
    return result.at[tuple(place)].set(high)


def raised(drawn, stream_key, source, target, shards_of, factor):
    def block_of(dim):
        return (jnp.arange(drawn.shape[dim]) // (drawn.shape[dim] // shards_of)).reshape((-1,) + (1,) * (drawn.ndim - 1 - dim))

    near = jax.random.permutation(stream_key, shards_of)[block_of(target)]
    other_side = (block_of(target) + shards_of // 2) % shards_of
    return jnp.where((block_of(source) == near) | (block_of(source) == other_side), factor * drawn, drawn)


def shard_levels(stream_key, dims, cuts, least, top_value):
    loudness = 1.0
    for axis_at, shards_of in cuts:
        heights = jax.random.uniform(jax.random.fold_in(jax.random.fold_in(stream_key, 6), axis_at), (shards_of,), jnp.float32, least / len(cuts), top_value / len(cuts))
        loudness = loudness * jnp.repeat(jnp.exp(heights), dims[axis_at] // shards_of).reshape((-1,) + (1,) * (len(dims) - 1 - axis_at))
    return loudness


def shared_out(stream_key, own, number, rows, number_of, top, most, lean):
    ranking = jax.random.permutation(stream_key, number_of)
    packed, usual = load_shares(number_of, rows * top, most, lean, True), load_shares(number_of, rows * top, most, lean, False)
    places = jnp.arange(number_of)

    def named(tallies, rotation):
        used = int((tallies > 0).sum())
        fixed = max(1, used // 4)
        passed = fixed + (places - fixed + rotation * (used - fixed)) % max(1, number_of - fixed)
        return jnp.zeros((number_of,), jnp.int32).at[ranking[jnp.where(places < fixed, places, passed)]].set(jnp.asarray(tallies, jnp.int32))

    tallies = jnp.where(number % 4 == 0, named(packed, number // 4), named(usual, number - number // 4 - 1))
    mixed = jax.random.permutation(jax.random.fold_in(own, 3), number_of)
    source_of, taker = mixed[0:number_of // 2 * 2:2], mixed[1:number_of // 2 * 2:2]
    slack = jnp.minimum(tallies[source_of] - 1, most - tallies[taker]) // 2
    slack = jnp.where((source_of == ranking[0]) | (taker == ranking[0]) | (tallies[taker] == 0), 0, jnp.maximum(slack, 0))
    passed = jax.random.randint(jax.random.fold_in(own, 4), (number_of // 2,), 0, 1 << 20) % (slack + 1)
    tallies = tallies.at[source_of].add(-passed).at[taker].add(passed)
    members = jnp.searchsorted(jnp.cumsum(tallies), jnp.arange(rows * top), side="right").astype(jnp.int32)
    listing = members.reshape(top, rows).T
    listing = listing[jax.random.permutation(jax.random.fold_in(own, 1), rows)]
    rotation = jax.random.randint(jax.random.fold_in(own, 2), (rows, 1), 0, top)
    return jnp.take_along_axis(listing, (jnp.arange(top)[None, :] + rotation) % top, axis=1)


def load_shares(amount, total, most, skew, full):
    loads = [(1 << 20) // math.isqrt(standing ** skew) + 1 for standing in range(1, amount + 1)]
    largest = most if full else min(most, max(-(-total // amount), total * loads[0] // sum(loads)))
    least = 1 if total - largest >= amount - 1 else 0
    holding, spare = [largest] + [least] * (amount - 1), total - largest - least * (amount - 1)
    while spare > 0:
        free = [i for i in range(1, amount) if holding[i] < largest] or [i for i in range(1, amount) if holding[i] < most]
        mass, budget = sum([loads[i] for i in free]), spare
        for i in free:
            addition = min(most - holding[i], max(1, budget * loads[i] // mass), spare)
            holding[i] = holding[i] + addition
            spare = spare - addition
    return np.array(holding)


def centred(stream_key, shape, deviation, bound, shards=(), kind=jnp.bfloat16):
    level = shard_levels(stream_key, shape, shards, -0.22, 0.18) if shards else 1.0
    entries = jax.random.normal(stream_key, shape, jnp.float32) * deviation * level
    return jnp.minimum(jnp.maximum(entries, -bound), bound).astype(kind)


def gaussian_with(rng, shape, spread, limit, shards, heavy, kind=jnp.bfloat16):
    entries = spread * jax.random.normal(rng, shape, jnp.float32)
    if shards:
        entries = entries * shard_levels(rng, shape, shards, -0.22, 0.18)
    return jnp.clip(raised(entries, jax.random.fold_in(rng, 3), *heavy), -limit, limit).astype(kind)


def setup_inputs(seed: int = 0) -> dict:
    streams_of = jax.random.split(jax.random.key(seed), 7)
    tokens = centred(streams_of[0], (TOKENS, D), 1.0, 6.0, ((0, 8), (1, 4)))
    routing_keys = jax.random.split(jax.random.fold_in(streams_of[1], 1), TOKENS // TOK_EP)
    routing_turns = jax.random.permutation(jax.random.fold_in(streams_of[1], 3), TOKENS // TOK_EP)
    routing = jax.vmap(lambda own, number: shared_out(jax.random.fold_in(streams_of[1], 2), own, number, TOK_EP, EXPERTS, TOP, CAP, 1))(routing_keys, routing_turns).reshape((TOKENS, TOP))
    gate_fixed = set_ends(jax.random.randint(streams_of[2], (TOKENS, TOP), 1, 65536), jax.random.fold_in(streams_of[2], 1), 1, 65535).astype(jnp.int32)
    gate_weight = centred(streams_of[3], (EXPERTS, D, FF), D ** -0.5, 0.125, ((0, 8), (1, 4)))
    up_weight = gaussian_with(streams_of[4], (EXPERTS, D, FF), D ** -0.5, 0.1875, ((0, 8), (1, 4)), (1, 2, 4, 2.0))
    down_weight = centred(streams_of[5], (EXPERTS, D, FF), FF ** -0.5, 0.21875, ((0, 8), (1, 4)))
    return dict(tokens=tokens, routing=routing, gate_fixed=gate_fixed, gate_weight=gate_weight, up_weight=up_weight, down_weight=down_weight)


def slot_positions(block_ids, experts):
    one_hot = (block_ids[..., None] == jnp.arange(experts, dtype=jnp.int32)).astype(jnp.int32)
    earlier = jnp.cumsum(one_hot, axis=1) - one_hot
    return jnp.sum(earlier * one_hot, axis=-1).astype(jnp.int32)


def expert_step(operands):
    slot_rows, gate_mat, up_mat, down_mat = operands
    gate_acts = jnp.dot(slot_rows, gate_mat, preferred_element_type=jnp.float32)
    up_acts = jnp.dot(slot_rows, up_mat, preferred_element_type=jnp.float32)
    hidden = (jax.nn.silu(gate_acts) * up_acts).astype(jnp.bfloat16)
    return jnp.dot(hidden, down_mat.T, preferred_element_type=jnp.float32).astype(jnp.bfloat16)


def reference(tokens, routing, gate_fixed, gate_weight, up_weight, down_weight):
    block_ids = routing.reshape(N_EP, TOK_EP * TOP).astype(jnp.int32)
    position = slot_positions(block_ids, EXPERTS)
    block_iota = jnp.broadcast_to(jnp.arange(N_EP, dtype=jnp.int32)[:, None], block_ids.shape)
    copies = jnp.repeat(tokens, TOP, axis=0).reshape(N_EP, TOK_EP * TOP, D)
    slot_rows = jnp.zeros((EXPERTS, N_EP, CAP, D), jnp.bfloat16)
    slot_rows = slot_rows.at[block_ids, block_iota, position].set(copies)
    results = lax.map(expert_step, (slot_rows.reshape(EXPERTS, N_EP * CAP, D), gate_weight, up_weight, down_weight))
    picked = results.reshape(EXPERTS, N_EP, CAP, D)[block_ids, block_iota, position]
    scales = (gate_fixed.astype(jnp.float32) / 65536.0).reshape(N_EP, TOK_EP * TOP, 1)
    mixed = (picked.astype(jnp.float32) * scales).reshape(TOKENS, TOP, D)
    return jnp.sum(mixed, axis=1).astype(jnp.bfloat16)
```

```python
import functools

import jax
import jax.numpy as jnp
from jax import lax
from jax.experimental import pallas as pl
from jax.experimental.pallas import tpu as pltpu
from jax.sharding import PartitionSpec as P

MESH = pl.DeviceIdType.MESH
SKEW = 2
GROUPS = 4
LANES = 128


def layer_kernel(
    nep, n, local, top, nq, half,
    tok_ref, meta_ref, gw_hbm, uw_hbm, dw_hbm,
    out_ref,
    gu, dw, tok_all, meta_all, place, ghi, glo, ends,
    xbuf, own, ra, rb, ha, hb, acc, out_send, out_recv,
    gu_sem, dw_sem, tok_s, tok_r, meta_s, meta_r,
    ra_s, ra_r, rb_s, rb_r, ha_s, ha_r, hb_s, hb_r, out_s, out_r,
):
    me = lax.axis_index("ep")
    z = lax.axis_index("tp")
    rows = tok_ref.shape[0]
    nb = nep // nq
    span = nb * rows
    ng = gu.shape[0]
    chunks = nq * ng
    bf16, f32 = jnp.bfloat16, jnp.float32
    zl = lax.rem(z + n - 1, n)
    zr = lax.rem(z + 1, n)
    my_group = me // nb
    my_slot = lax.rem(me, nb)

    def gate_copy(g):
        return pltpu.make_async_copy(
            gw_hbm.at[:, :, pl.ds(g * LANES, LANES)],
            gu.at[g, :, :, pl.ds(0, LANES)], gu_sem.at[0, g],
        )

    def up_copy(g):
        return pltpu.make_async_copy(
            uw_hbm.at[:, :, pl.ds(g * LANES, LANES)],
            gu.at[g, :, :, pl.ds(LANES, LANES)], gu_sem.at[1, g],
        )

    down_copy = pltpu.make_async_copy(dw_hbm, dw, dw_sem)

    for g in range(ng):
        gate_copy(g).start()
        up_copy(g).start()
    down_copy.start()

    barrier = pltpu.get_barrier_semaphore()

    def greet(j, carry):
        pl.semaphore_signal(
            barrier, inc=1, device_id={"ep": lax.rem(me + j, nep)}, device_id_type=MESH
        )
        return carry

    lax.fori_loop(1, nep, greet, 0)
    for side in (zl, zr):
        pl.semaphore_signal(barrier, inc=1, device_id={"tp": side}, device_id_type=MESH)
    pl.semaphore_wait(barrier, nep + 1)

    def remote(src, dst, s, r, device):
        return pltpu.make_async_remote_copy(
            src_ref=src, dst_ref=dst, send_sem=s, recv_sem=r,
            device_id=device, device_id_type=MESH,
        )

    def block_of(i):
        return pl.ds(pl.multiple_of(i * rows, rows), rows)

    def tok_copy(m):
        to = lax.rem(my_group - m // nb + nq, nq) * nb + lax.rem(m, nb)
        slot = (m // nb) * nb + my_slot
        return remote(
            tok_ref, tok_all.at[m // nb, block_of(my_slot), :], tok_s.at[m], tok_r.at[slot],
            {"ep": to},
        )

    def meta_copy(m):
        to = lax.rem(my_group - m // nb + nq, nq) * nb + lax.rem(m, nb)
        slot = (m // nb) * nb + my_slot
        return remote(
            meta_ref, meta_all.at[m // nb, :, block_of(my_slot)], meta_s.at[m], meta_r.at[slot],
            {"ep": to},
        )

    def tok_arrival(m):
        return remote(
            tok_ref, tok_all.at[m // nb, block_of(lax.rem(m, nb)), :], tok_s.at[m], tok_r.at[m],
            {"ep": lax.rem(me + 1, nep)},
        )

    def meta_arrival(m):
        return remote(
            meta_ref, meta_all.at[m // nb, :, block_of(lax.rem(m, nb))], meta_s.at[m],
            meta_r.at[m], {"ep": lax.rem(me + 1, nep)},
        )

    def out_copy(m):
        to = lax.rem(my_group + m // nb, nq) * nb + lax.rem(m, nb)
        return remote(
            out_send.at[m // nb, block_of(lax.rem(m, nb)), :], out_recv.at[me],
            out_s.at[m], out_r.at[me], {"ep": to},
        )

    def out_arrival(j):
        source = lax.rem(me + j, nep)
        return source, remote(
            out_send.at[0, block_of(0), :], out_recv.at[source],
            out_s.at[0], out_r.at[source], {"ep": source},
        )

    def ra_copy(k):
        return remote(ra.at[k], ra.at[k], ra_s.at[k], ra_r.at[k], {"tp": zl})

    def rb_copy(k):
        return remote(rb.at[k], rb.at[k], rb_s.at[k], rb_r.at[k], {"tp": zr})

    def ha_copy(k):
        return remote(ha.at[k], ha.at[k], ha_s.at[k], ha_r.at[k], {"tp": zr})

    def hb_copy(k):
        return remote(hb.at[k], hb.at[k], hb_s.at[k], hb_r.at[k], {"tp": zl})

    def send_tokens(m, carry):
        @pl.when(m != my_slot)
        def _():
            meta_copy(m).start()
            tok_copy(m).start()

        return carry

    lax.fori_loop(0, nep, send_tokens, 0)
    tok_all[0, block_of(my_slot), :] = tok_ref[...]
    meta_all[0, :, block_of(my_slot)] = meta_ref[...]

    def clear(j, carry):
        acc[j] = jnp.zeros(acc.shape[1:], acc.dtype)
        return carry

    lax.fori_loop(0, nq, clear, 0)

    before = (
        lax.broadcasted_iota(jnp.int32, (span, span), 0)
        < lax.broadcasted_iota(jnp.int32, (span, span), 1)
    ).astype(bf16)
    row_id = lax.broadcasted_iota(jnp.int32, (half, span), 0).astype(f32)
    row_col = lax.broadcasted_iota(jnp.int32, (half, LANES), 0).astype(f32)
    sub_id = lax.broadcasted_iota(jnp.int32, (16, span), 0)

    def prepare(q):
        def arrive(i, carry):
            m = q * nb + i

            @pl.when(m != my_slot)
            def _():
                meta_arrival(m).wait_recv()
                tok_arrival(m).wait_recv()

            return carry

        lax.fori_loop(0, nb, arrive, 0)
        ids = meta_all[q, :top, :]
        fixed = meta_all[q, top:, :]
        chosen, wide = [], jnp.zeros((16, span), f32)
        for e in range(local):
            named = ids == me * local + e
            row = jnp.sum(named.astype(f32), axis=0, keepdims=True)
            gate = jnp.sum(jnp.where(named, fixed, 0), axis=0, keepdims=True)
            high = gate // 256
            ghi[q, e:e + 1, :] = (high * 256).astype(f32)
            glo[q, e:e + 1, :] = (gate - high * 256).astype(f32)
            wide = jnp.where(sub_id == e, row, wide)
            chosen.append(row)
        earlier = jnp.dot(wide.astype(bf16), before, preferred_element_type=f32)
        base = jnp.zeros((1, 1), f32)
        for e in range(local):
            place[q, e:e + 1, :] = jnp.where(
                chosen[e] > 0.5, base + earlier[e:e + 1, :], -1.0
            )
            base = base + jnp.sum(chosen[e], axis=1, keepdims=True)
            ends[q, e:e + 1, :] = jnp.broadcast_to(base, (1, LANES))

    def inside(k):
        return jnp.logical_and(k >= 0, k < chunks)

    def partial_stage(k, d, buf, copy, has_source, is_last, hidden):
        @pl.when(inside(k))
        def _():
            q = k // ng
            g = lax.rem(k, ng)

            @pl.when(g == 0)
            def _():
                for e in range(local):
                    pick = (row_id + float(d * half)) == place[q, e:e + 1, :]
                    xbuf[d, e] = jnp.dot(
                        pick.astype(bf16), tok_all[q], preferred_element_type=f32
                    ).astype(bf16)

            total = jnp.dot(xbuf[d, 0], gu[g, 0], preferred_element_type=f32)
            for e in range(1, local):
                total += jnp.dot(xbuf[d, e], gu[g, e], preferred_element_type=f32)
            own[...] = total

            @pl.when(has_source)
            def _():
                copy(k).wait_recv()
                own[...] += buf[k].astype(f32)

            @pl.when(jnp.logical_not(is_last))
            def _():
                buf[k] = own[...].astype(bf16)
                copy(k).start()

            @pl.when(is_last)
            def _():
                v = own[:, :LANES]
                hidden[k] = (v / (1.0 + jnp.exp(-v)) * own[:, LANES:]).astype(bf16)

    def hidden_stage(k, d, hidden, copy, has_source, is_last):
        @pl.when(inside(k))
        def _():
            @pl.when(has_source)
            def _():
                copy(k).wait_recv()

            @pl.when(jnp.logical_not(is_last))
            def _():
                copy(k).start()

            q = k // ng

            @pl.when(lax.rem(k, ng) == ng - 1)
            def _():
                units = jnp.concatenate([hidden[q * ng + g] for g in range(ng)], axis=1)
                at = row_col + float(d * half)
                start = jnp.zeros((1, LANES), f32)
                result = jnp.zeros((half, dw.shape[1]), f32)
                high = jnp.zeros((half, span), f32)
                low = jnp.zeros((half, span), f32)
                for e in range(local):
                    end = ends[q, e:e + 1, :]
                    mine = jnp.logical_and(at >= start, at < end).astype(f32).astype(bf16)
                    start = end
                    result += lax.dot_general(
                        units * jnp.concatenate([mine] * ng, axis=1), dw[e],
                        (((1,), (1,)), ((), ())), preferred_element_type=f32,
                    )
                    pick = (row_id + float(d * half)) == place[q, e:e + 1, :]
                    high = jnp.where(pick, ghi[q, e:e + 1, :], high)
                    low = jnp.where(pick, glo[q, e:e + 1, :], low)
                rounded = result.astype(bf16)
                acc[q] += lax.dot_general(
                    jnp.concatenate([high.astype(bf16), low.astype(bf16)], axis=0),
                    jnp.concatenate([rounded, rounded], axis=0),
                    (((0,), (0,)), ((), ())), preferred_element_type=f32,
                )

    turn = SKEW * (n - 1)
    from_right = SKEW * (n - 1 - z)
    from_left = SKEW * z
    lead = jnp.minimum(from_left, from_right)

    def step(t, carry):
        k_first = t - lead

        @pl.when(jnp.logical_and(inside(k_first), lax.rem(k_first, ng) == 0))
        def _():
            prepare(k_first // ng)

        @pl.when(jnp.logical_and(k_first >= 0, k_first < ng))
        def _():
            gate_copy(k_first).wait()
            up_copy(k_first).wait()

        @pl.when(t == turn + lead)
        def _():
            down_copy.wait()

        partial_stage(t - from_right, 0, ra, ra_copy, z < n - 1, z == 0, ha)
        partial_stage(t - from_left, 1, rb, rb_copy, z > 0, z == n - 1, hb)
        hidden_stage(t - turn - from_left, 0, ha, ha_copy, z > 0, z == n - 1)
        hidden_stage(t - turn - from_right, 1, hb, hb_copy, z < n - 1, z == 0)
        k_done = t - turn - jnp.maximum(from_left, from_right)

        @pl.when(jnp.logical_and(inside(k_done), lax.rem(k_done, ng) == ng - 1))
        def _():
            q = k_done // ng
            out_send[q] = (acc[q] * (1.0 / 65536.0)).astype(bf16)

            def give(i, carry):
                m = q * nb + i

                @pl.when(m != my_slot)
                def _():
                    out_copy(m).start()

                return carry

            lax.fori_loop(0, nb, give, 0)

        return carry

    lax.fori_loop(0, chunks + 2 * turn, step, 0)

    def finish_chunk(k, carry):
        @pl.when(z > 0)
        def _():
            ra_copy(k).wait_send()
            hb_copy(k).wait_send()

        @pl.when(z < n - 1)
        def _():
            rb_copy(k).wait_send()
            ha_copy(k).wait_send()

        return carry

    lax.fori_loop(0, chunks, finish_chunk, 0)

    def finish_send(m, carry):
        @pl.when(m != my_slot)
        def _():
            tok_copy(m).wait_send()
            meta_copy(m).wait_send()
            out_copy(m).wait_send()

        return carry

    lax.fori_loop(0, nep, finish_send, 0)
    own_rows = block_of(my_slot)
    acc[0, own_rows, :] = acc[0, own_rows, :] * (1.0 / 65536.0)

    def finish_block(j, carry):
        source, copy = out_arrival(j)
        copy.wait_recv()
        acc[0, own_rows, :] += out_recv[source].astype(f32)
        return carry

    lax.fori_loop(1, nep, finish_block, 0)
    out_ref[...] = acc[0, own_rows, :].astype(bf16)


def on_device(nep, n, tokens, routing, gate_fixed, gate_weight, up_weight, down_weight):
    local, share, width = gate_weight.shape
    rows, top = routing.shape
    cap = max(2, rows * top * 2 // (local * nep))
    nq = min(GROUPS, nep)
    nb = nep // nq
    half = nb * local * cap // 2
    ng = width // LANES
    chunks = nq * ng
    meta = jnp.concatenate([routing.T, gate_fixed.T], axis=0)
    bf16, f32 = jnp.bfloat16, jnp.float32
    dma = pltpu.SemaphoreType.DMA
    vmem = pl.BlockSpec(memory_space=pltpu.VMEM)
    hbm = pl.BlockSpec(memory_space=pl.ANY)
    return pl.pallas_call(
        functools.partial(layer_kernel, nep, n, local, top, nq, half),
        out_shape=jax.ShapeDtypeStruct((rows, share), bf16),
        in_specs=[vmem, vmem, hbm, hbm, hbm],
        out_specs=vmem,
        scratch_shapes=[
            pltpu.VMEM((ng, local, share, 2 * LANES), bf16),
            pltpu.VMEM((local, share, width), bf16),
            pltpu.VMEM((nq, nb * rows, share), bf16),
            pltpu.VMEM((nq, 2 * top, nb * rows), jnp.int32),
            pltpu.VMEM((nq, 8, nb * rows), f32),
            pltpu.VMEM((nq, 8, nb * rows), f32),
            pltpu.VMEM((nq, 8, nb * rows), f32),
            pltpu.VMEM((nq, 8, LANES), f32),
            pltpu.VMEM((2, local, half, share), bf16),
            pltpu.VMEM((half, 2 * LANES), f32),
            pltpu.VMEM((chunks, half, 2 * LANES), bf16),
            pltpu.VMEM((chunks, half, 2 * LANES), bf16),
            pltpu.VMEM((chunks, half, LANES), bf16),
            pltpu.VMEM((chunks, half, LANES), bf16),
            pltpu.VMEM((nq, nb * rows, share), f32),
            pltpu.VMEM((nq, nb * rows, share), bf16),
            pltpu.VMEM((nep, rows, share), bf16),
            dma((2, ng)), dma,
            dma((nep,)), dma((nep,)), dma((nep,)), dma((nep,)),
            dma((chunks,)), dma((chunks,)), dma((chunks,)), dma((chunks,)),
            dma((chunks,)), dma((chunks,)), dma((chunks,)), dma((chunks,)),
            dma((nep,)), dma((nep,)),
        ],
        compiler_params=pltpu.CompilerParams(
            collective_id=0, has_side_effects=True, vmem_limit_bytes=60 * 1024 * 1024
        ),
    )(tokens, meta, gate_weight, up_weight, down_weight)


def solution(mesh):
    in_specs = (
        P("ep", "tp"),
        P("ep", None),
        P("ep", None),
        P("ep", "tp", None),
        P("ep", "tp", None),
        P("ep", "tp", None),
    )
    body = functools.partial(on_device, mesh.shape["ep"], mesh.shape["tp"])
    return jax.shard_map(
        body, mesh=mesh, in_specs=in_specs, out_specs=P("ep", "tp"), check_vma=False
    )
```

```python
import functools

import jax
import jax.numpy as jnp
from jax import lax
from jax.experimental import pallas as pl
from jax.experimental.pallas import tpu as pltpu
from jax.sharding import PartitionSpec as P

MESH = pl.DeviceIdType.MESH
SKEW = 2
GROUPS = 4
LANES = 128
SIZES = (10, 11)


def remote(src, dst, s, r, device):
    return pltpu.make_async_remote_copy(
        src_ref=src, dst_ref=dst, send_sem=s, recv_sem=r,
        device_id=device, device_id_type=MESH,
    )


def count_kernel(
    nep, nq, local, top, limits,
    meta_ref, all_ref, size_ref, meta_all, meta_s, meta_r,
):
    me = lax.axis_index("ep")
    rows = meta_ref.shape[1]
    nb = nep // nq
    my_group = me // nb
    my_slot = lax.rem(me, nb)
    barrier = pltpu.get_barrier_semaphore()

    def greet(j, carry):
        pl.semaphore_signal(
            barrier, inc=1, device_id={"ep": lax.rem(me + j, nep)}, device_id_type=MESH
        )
        return carry

    lax.fori_loop(1, nep, greet, 0)
    pl.semaphore_wait(barrier, nep - 1)

    def block_of(i):
        return pl.ds(pl.multiple_of(i * rows, rows), rows)

    def give(m):
        to = lax.rem(my_group - m // nb + nq, nq) * nb + lax.rem(m, nb)
        slot = (m // nb) * nb + my_slot
        return remote(
            meta_ref, meta_all.at[m // nb, :, block_of(my_slot)], meta_s.at[m], meta_r.at[slot],
            {"ep": to},
        )

    def arrival(m):
        return remote(
            meta_ref, meta_all.at[m // nb, :, block_of(lax.rem(m, nb))], meta_s.at[m],
            meta_r.at[m], {"ep": lax.rem(me + 1, nep)},
        )

    def start(m, carry):
        @pl.when(m != my_slot)
        def _():
            give(m).start()

        return carry

    def finish(m, carry):
        @pl.when(m != my_slot)
        def _():
            arrival(m).wait_recv()

        return carry

    def sent(m, carry):
        @pl.when(m != my_slot)
        def _():
            give(m).wait_send()

        return carry

    lax.fori_loop(0, nep, start, 0)
    meta_all[0, :, block_of(my_slot)] = meta_ref[...]
    lax.fori_loop(0, nep, finish, 0)
    worst = jnp.zeros((1, 1), jnp.float32)
    for q in range(nq):
        ids = meta_all[q, :top, :]
        all_ref[q] = meta_all[q]
        for c in range(nep // 2):
            here = jnp.logical_and(ids >= c * 2 * local, ids < (c + 1) * 2 * local)
            row = jnp.sum(here.astype(jnp.float32), axis=0, keepdims=True)
            worst = jnp.maximum(worst, jnp.sum(row, axis=1, keepdims=True))
    top_load = jnp.max(worst)
    size = jnp.int32(0)
    for limit in limits:
        size += (top_load > float(limit)).astype(jnp.int32)
    size_ref[0] = size
    lax.fori_loop(0, nep, sent, 0)


def layer_kernel(
    nep, n, local, top, nq, full, half,
    tok_ref, meta_all, gw_hbm, uw_hbm, dw_hbm,
    out_ref,
    gu, dw, tok_all, place, gate, ends,
    xbuf, own, ra, rb, ha, hb, sp_out, sp_in, hs_in, acc, out_send, out_recv,
    gu_sem, dw_sem, tok_s, tok_r,
    ra_s, ra_r, rb_s, rb_r, ha_s, ha_r, hb_s, hb_r, sp_s, sp_r, hs_s, hs_r, out_s, out_r,
):
    me = lax.axis_index("ep")
    z = lax.axis_index("tp")
    spill = full - half
    low_row = half - spill
    partner = me + 1 - 2 * lax.rem(me, 2)
    rows = tok_ref.shape[0]
    nb = nep // nq
    span = nb * rows
    ng = gu.shape[0]
    chunks = nq * ng
    bf16, f32 = jnp.bfloat16, jnp.float32
    zl = lax.rem(z + n - 1, n)
    zr = lax.rem(z + 1, n)
    my_group = me // nb
    my_slot = lax.rem(me, nb)

    def gate_copy(g):
        return pltpu.make_async_copy(
            gw_hbm.at[:, :, pl.ds(g * LANES, LANES)],
            gu.at[g, :, :, pl.ds(0, LANES)], gu_sem.at[0, g],
        )

    def up_copy(g):
        return pltpu.make_async_copy(
            uw_hbm.at[:, :, pl.ds(g * LANES, LANES)],
            gu.at[g, :, :, pl.ds(LANES, LANES)], gu_sem.at[1, g],
        )

    down_copy = pltpu.make_async_copy(dw_hbm, dw, dw_sem)

    for g in range(ng):
        gate_copy(g).start()
        up_copy(g).start()
    down_copy.start()

    barrier = pltpu.get_barrier_semaphore()

    def greet(j, carry):
        pl.semaphore_signal(
            barrier, inc=1, device_id={"ep": lax.rem(me + j, nep)}, device_id_type=MESH
        )
        return carry

    lax.fori_loop(1, nep, greet, 0)
    for side in (zl, zr):
        pl.semaphore_signal(barrier, inc=1, device_id={"tp": side}, device_id_type=MESH)
    pl.semaphore_wait(barrier, nep + 1)

    def block_of(i):
        return pl.ds(pl.multiple_of(i * rows, rows), rows)

    def tok_copy(m):
        to = lax.rem(my_group - m // nb + nq, nq) * nb + lax.rem(m, nb)
        slot = (m // nb) * nb + my_slot
        return remote(
            tok_ref, tok_all.at[m // nb, block_of(my_slot), :], tok_s.at[m], tok_r.at[slot],
            {"ep": to},
        )

    def tok_arrival(m):
        return remote(
            tok_ref, tok_all.at[m // nb, block_of(lax.rem(m, nb)), :], tok_s.at[m], tok_r.at[m],
            {"ep": lax.rem(me + 1, nep)},
        )

    def out_copy(m):
        to = lax.rem(my_group + m // nb, nq) * nb + lax.rem(m, nb)
        return remote(
            out_send.at[m // nb, block_of(lax.rem(m, nb)), :], out_recv.at[me],
            out_s.at[m], out_r.at[me], {"ep": to},
        )

    def out_arrival(j):
        source = lax.rem(me + j, nep)
        return source, remote(
            out_send.at[0, block_of(0), :], out_recv.at[source],
            out_s.at[0], out_r.at[source], {"ep": source},
        )

    def ra_copy(k):
        return remote(ra.at[k], ra.at[k], ra_s.at[k], ra_r.at[k], {"tp": zl})

    def rb_copy(k):
        return remote(rb.at[k], rb.at[k], rb_s.at[k], rb_r.at[k], {"tp": zr})

    def ha_copy(k):
        return remote(ha.at[k], ha.at[k], ha_s.at[k], ha_r.at[k], {"tp": zr})

    def hb_copy(k):
        return remote(hb.at[k], hb.at[k], hb_s.at[k], hb_r.at[k], {"tp": zl})

    def send_tokens(m, carry):
        @pl.when(m != my_slot)
        def _():
            tok_copy(m).start()

        return carry

    lax.fori_loop(0, nep, send_tokens, 0)
    tok_all[0, block_of(my_slot), :] = tok_ref[...]

    def clear(j, carry):
        acc[j] = jnp.zeros(acc.shape[1:], acc.dtype)
        return carry

    lax.fori_loop(0, nq, clear, 0)

    before = (
        lax.broadcasted_iota(jnp.int32, (span, span), 0)
        < lax.broadcasted_iota(jnp.int32, (span, span), 1)
    ).astype(bf16)

    def row_ids(d, lanes):
        r = lax.broadcasted_iota(jnp.int32, (full, lanes), 0)
        mine = 2 * r + d
        lent = 2 * full - 1 - d - 2 * (r - half)
        return jnp.where(r < half, mine, lent).astype(f32)
    sub_id = lax.broadcasted_iota(jnp.int32, (16, span), 0)

    def prepare(q):
        def arrive(i, carry):
            m = q * nb + i

            @pl.when(m != my_slot)
            def _():
                tok_arrival(m).wait_recv()

            return carry

        lax.fori_loop(0, nb, arrive, 0)
        ids = meta_all[q, :top, :]
        fixed = meta_all[q, top:, :]
        chosen, wide = [], jnp.zeros((16, span), f32)
        for e in range(local):
            named = ids == me * local + e
            row = jnp.sum(named.astype(f32), axis=0, keepdims=True)
            weight = jnp.sum(jnp.where(named, fixed, 0), axis=0, keepdims=True)
            gate[q, e:e + 1, :] = weight.astype(f32) * (1.0 / 65536.0)
            wide = jnp.where(sub_id == e, row, wide)
            chosen.append(row)
        earlier = jnp.dot(wide.astype(bf16), before, preferred_element_type=f32)
        base = jnp.zeros((1, 1), f32)
        for e in range(local):
            place[q, e:e + 1, :] = jnp.where(
                chosen[e] > 0.5, base + earlier[e:e + 1, :], -1.0
            )
            base = base + jnp.sum(chosen[e], axis=1, keepdims=True)
            ends[q, e:e + 1, :] = jnp.broadcast_to(base, (1, LANES))

    def inside(k):
        return jnp.logical_and(k >= 0, k < chunks)

    def lend_copy(k, d):
        i = d * chunks + k
        return remote(sp_out.at[i], sp_in.at[i], sp_s.at[i], sp_r.at[i], {"ep": partner})

    def back_copy(k, d, hidden):
        i = d * chunks + k
        return remote(
            hidden.at[k, pl.ds(low_row, spill), :], hs_in.at[i], hs_s.at[i], hs_r.at[i],
            {"ep": partner},
        )

    def product_stage(k, d):
        @pl.when(inside(k))
        def _():
            q = k // ng
            g = lax.rem(k, ng)

            @pl.when(g == 0)
            def _():
                ids = row_ids(d, span)
                for e in range(local):
                    pick = ids == place[q, e:e + 1, :]
                    xbuf[d, e] = jnp.dot(
                        pick.astype(bf16), tok_all[q], preferred_element_type=f32
                    ).astype(bf16)

            total = jnp.dot(xbuf[d, 0], gu[g, 0], preferred_element_type=f32)
            for e in range(1, local):
                total += jnp.dot(xbuf[d, e], gu[g, e], preferred_element_type=f32)
            own[d, lax.rem(k, 2)] = total[:half]
            if spill:
                sp_out[d * chunks + k] = total[half:]
                lend_copy(k, d).start()

    def chain_stage(k, d, buf, copy, has_source, is_last, hidden):
        @pl.when(inside(k))
        def _():
            mine = own.at[d, lax.rem(k, 2)]
            if spill:
                lend_copy(k, d).wait_recv()
                mine[low_row:, :] += sp_in[d * chunks + k]

            @pl.when(has_source)
            def _():
                copy(k).wait_recv()
                mine[...] += buf[k].astype(f32)

            @pl.when(jnp.logical_not(is_last))
            def _():
                buf[k] = mine[...].astype(bf16)
                copy(k).start()

            @pl.when(is_last)
            def _():
                v = mine[:, :LANES]
                hidden[k] = (v / (1.0 + jnp.exp(-v)) * mine[:, LANES:]).astype(bf16)

    def hidden_stage(k, d, hidden, copy, has_source, is_last):
        @pl.when(inside(k))
        def _():
            @pl.when(has_source)
            def _():
                copy(k).wait_recv()

            @pl.when(jnp.logical_not(is_last))
            def _():
                copy(k).start()

            if spill:
                back_copy(k, d, hidden).start()

    def down_stage(k, d, hidden):
        @pl.when(inside(k))
        def _():
            if spill:
                back_copy(k, d, hidden).wait_recv()
            q = k // ng

            @pl.when(lax.rem(k, ng) == ng - 1)
            def _():
                units = jnp.concatenate([hidden[q * ng + g] for g in range(ng)], axis=1)
                if spill:
                    lent = jnp.concatenate(
                        [hs_in[d * chunks + q * ng + g] for g in range(ng)], axis=1
                    )
                    units = jnp.concatenate([units, lent], axis=0)
                at = row_ids(d, LANES)
                ids = row_ids(d, span)
                start = jnp.zeros((1, LANES), f32)
                result = jnp.zeros((full, dw.shape[1]), f32)
                spread = jnp.zeros((full, span), f32)
                scale = jnp.zeros((full, span), f32)
                for e in range(local):
                    end = ends[q, e:e + 1, :]
                    mine = jnp.logical_and(at >= start, at < end).astype(f32).astype(bf16)
                    start = end
                    result += lax.dot_general(
                        units * jnp.concatenate([mine] * ng, axis=1), dw[e],
                        (((1,), (1,)), ((), ())), preferred_element_type=f32,
                    )
                    pick = ids == place[q, e:e + 1, :]
                    spread = jnp.where(pick, 1.0, spread)
                    scale = jnp.where(pick, gate[q, e:e + 1, :], scale)
                scaled = result * jnp.sum(scale, axis=1, keepdims=True)
                high = scaled.astype(bf16)
                low = (scaled - high.astype(f32)).astype(bf16)
                spread = spread.astype(bf16)
                acc[q] += lax.dot_general(
                    jnp.concatenate([spread, spread], axis=0),
                    jnp.concatenate([high, low], axis=0),
                    (((0,), (0,)), ((), ())), preferred_element_type=f32,
                )

    turn = SKEW * (n - 1)
    from_right = SKEW * (n - 1 - z)
    from_left = SKEW * z
    lead = jnp.minimum(from_left, from_right)

    def step(t, carry):
        k_first = t - lead

        @pl.when(jnp.logical_and(inside(k_first), lax.rem(k_first, ng) == 0))
        def _():
            prepare(k_first // ng)

        @pl.when(jnp.logical_and(k_first >= 0, k_first < ng))
        def _():
            gate_copy(k_first).wait()
            up_copy(k_first).wait()

        @pl.when(t == turn + lead + 1)
        def _():
            down_copy.wait()

        product_stage(t - from_right, 0)
        product_stage(t - from_left, 1)
        chain_stage(t - 1 - from_right, 0, ra, ra_copy, z < n - 1, z == 0, ha)
        chain_stage(t - 1 - from_left, 1, rb, rb_copy, z > 0, z == n - 1, hb)
        hidden_stage(t - 1 - turn - from_left, 0, ha, ha_copy, z > 0, z == n - 1)
        hidden_stage(t - 1 - turn - from_right, 1, hb, hb_copy, z < n - 1, z == 0)
        down_stage(t - 2 - turn - from_left, 0, ha)
        down_stage(t - 2 - turn - from_right, 1, hb)
        k_done = t - 2 - turn - jnp.maximum(from_left, from_right)

        @pl.when(jnp.logical_and(inside(k_done), lax.rem(k_done, ng) == ng - 1))
        def _():
            q = k_done // ng
            out_send[q] = acc[q].astype(bf16)

            def give(i, carry):
                m = q * nb + i

                @pl.when(m != my_slot)
                def _():
                    out_copy(m).start()

                return carry

            lax.fori_loop(0, nb, give, 0)

        return carry

    lax.fori_loop(0, chunks + 2 * turn + 2, step, 0)

    def finish_chunk(k, carry):
        if spill:
            lend_copy(k, 0).wait_send()
            lend_copy(k, 1).wait_send()
            back_copy(k, 0, ha).wait_send()
            back_copy(k, 1, hb).wait_send()

        @pl.when(z > 0)
        def _():
            ra_copy(k).wait_send()
            hb_copy(k).wait_send()

        @pl.when(z < n - 1)
        def _():
            rb_copy(k).wait_send()
            ha_copy(k).wait_send()

        return carry

    lax.fori_loop(0, chunks, finish_chunk, 0)

    def finish_send(m, carry):
        @pl.when(m != my_slot)
        def _():
            tok_copy(m).wait_send()
            out_copy(m).wait_send()

        return carry

    lax.fori_loop(0, nep, finish_send, 0)
    own_rows = block_of(my_slot)

    def finish_block(j, carry):
        source, copy = out_arrival(j)
        copy.wait_recv()
        acc[0, own_rows, :] += out_recv[source].astype(f32)
        return carry

    lax.fori_loop(1, nep, finish_block, 0)
    out_ref[...] = acc[0, own_rows, :].astype(bf16)


def count_call(nep, nq, local, limits, meta):
    depth, rows = meta.shape
    nb = nep // nq
    dma = pltpu.SemaphoreType.DMA
    vmem = pl.BlockSpec(memory_space=pltpu.VMEM)
    shape = (nq, depth, nb * rows)
    return pl.pallas_call(
        functools.partial(count_kernel, nep, nq, local, depth // 2, limits),
        out_shape=(
            jax.ShapeDtypeStruct(shape, jnp.int32), jax.ShapeDtypeStruct((1,), jnp.int32)
        ),
        in_specs=[vmem],
        out_specs=(vmem, pl.BlockSpec(memory_space=pltpu.SMEM)),
        scratch_shapes=[pltpu.VMEM(shape, jnp.int32), dma((nep,)), dma((nep,))],
        compiler_params=pltpu.CompilerParams(collective_id=0, has_side_effects=True),
    )(meta)


def layer_call(nep, n, nq, top, full, half, number, tokens, meta_all, gate_weight, up_weight, down_weight):
    local, share, width = gate_weight.shape
    rows = tokens.shape[0]
    nb = nep // nq
    ng = width // LANES
    chunks = nq * ng
    spill = max(full - half, 16)
    lent = 2 * chunks if half < full else 1
    bf16, f32 = jnp.bfloat16, jnp.float32
    dma = pltpu.SemaphoreType.DMA
    vmem = pl.BlockSpec(memory_space=pltpu.VMEM)
    hbm = pl.BlockSpec(memory_space=pl.ANY)
    return pl.pallas_call(
        functools.partial(layer_kernel, nep, n, local, top, nq, full, half),
        out_shape=jax.ShapeDtypeStruct((rows, share), bf16),
        in_specs=[vmem, vmem, hbm, hbm, hbm],
        out_specs=vmem,
        scratch_shapes=[
            pltpu.VMEM((ng, local, share, 2 * LANES), bf16),
            pltpu.VMEM((local, share, width), bf16),
            pltpu.VMEM((nq, nb * rows, share), bf16),
            pltpu.VMEM((nq, 8, nb * rows), f32),
            pltpu.VMEM((nq, 8, nb * rows), f32),
            pltpu.VMEM((nq, 8, LANES), f32),
            pltpu.VMEM((2, local, full, share), bf16),
            pltpu.VMEM((2, 2, half, 2 * LANES), f32),
            pltpu.VMEM((chunks, half, 2 * LANES), bf16),
            pltpu.VMEM((chunks, half, 2 * LANES), bf16),
            pltpu.VMEM((chunks, half, LANES), bf16),
            pltpu.VMEM((chunks, half, LANES), bf16),
            pltpu.VMEM((lent, spill, 2 * LANES), f32),
            pltpu.VMEM((lent, spill, 2 * LANES), f32),
            pltpu.VMEM((lent, spill, LANES), bf16),
            pltpu.VMEM((nq, nb * rows, share), f32),
            pltpu.VMEM((nq, nb * rows, share), bf16),
            pltpu.VMEM((nep, rows, share), bf16),
            dma((2, ng)), dma,
            dma((nep,)), dma((nep,)),
            dma((chunks,)), dma((chunks,)), dma((chunks,)), dma((chunks,)),
            dma((chunks,)), dma((chunks,)), dma((chunks,)), dma((chunks,)),
            dma((lent,)), dma((lent,)), dma((lent,)), dma((lent,)),
            dma((nep,)), dma((nep,)),
        ],
        compiler_params=pltpu.CompilerParams(
            collective_id=number, has_side_effects=True, vmem_limit_bytes=60 * 1024 * 1024
        ),
    )(tokens, meta_all, gate_weight, up_weight, down_weight)


def on_device(nep, n, tokens, routing, gate_fixed, gate_weight, up_weight, down_weight):
    local = gate_weight.shape[0]
    rows, top = routing.shape
    cap = max(2, rows * top * 2 // (local * nep))
    nq = min(GROUPS, nep)
    full = nep // nq * local * cap // 2
    halves = [h for h in (full * s // 16 for s in SIZES) if h % 16 == 0] + [full]
    meta = jnp.concatenate([routing.T, gate_fixed.T], axis=0)
    meta_all, size = count_call(nep, nq, local, [4 * h for h in halves[:-1]], meta)
    calls = [
        functools.partial(layer_call, nep, n, nq, top, full, h, i + 1)
        for i, h in enumerate(halves)
    ]
    return lax.switch(
        size[0], calls, tokens, meta_all, gate_weight, up_weight, down_weight
    )


def solution(mesh):
    in_specs = (
        P("ep", "tp"),
        P("ep", None),
        P("ep", None),
        P("ep", "tp", None),
        P("ep", "tp", None),
        P("ep", "tp", None),
    )
    body = functools.partial(on_device, mesh.shape["ep"], mesh.shape["tp"])
    return jax.shard_map(
        body, mesh=mesh, in_specs=in_specs, out_specs=P("ep", "tp"), check_vma=False
    )
```

```python
import functools

import jax
import jax.numpy as jnp
from jax import lax
from jax.experimental import pallas as pl
from jax.experimental.pallas import tpu as pltpu
from jax.sharding import PartitionSpec as P

MESH = pl.DeviceIdType.MESH
SKEW = 2
LEAD = 2
LATE = 1
GROUPS = 4
LANES = 128
SIZES = (18, 19, 20, 21, 22)


def remote(src, dst, s, r, device):
    return pltpu.make_async_remote_copy(
        src_ref=src, dst_ref=dst, send_sem=s, recv_sem=r,
        device_id=device, device_id_type=MESH,
    )


def count_kernel(
    nep, nq, local, top, limits,
    ids_ref, gate_ref, all_ref, size_ref, meta_ref, meta_all, meta_s, meta_r,
):
    me = lax.axis_index("ep")
    rows = meta_ref.shape[1]
    nb = nep // nq
    span = nb * rows
    my_group = me // nb
    my_slot = lax.rem(me, nb)
    barrier = pltpu.get_barrier_semaphore()

    def greet(j, carry):
        pl.semaphore_signal(
            barrier, inc=1, device_id={"ep": lax.rem(me + j, nep)}, device_id_type=MESH
        )
        return carry

    lax.fori_loop(1, nep, greet, 0)
    meta_ref[:top] = ids_ref[...]
    meta_ref[top:] = gate_ref[...]
    pl.semaphore_wait(barrier, nep - 1)

    def block_of(i):
        return pl.ds(pl.multiple_of(i * rows, rows), rows)

    def give(m):
        to = lax.rem(my_group - m // nb + nq, nq) * nb + lax.rem(m, nb)
        slot = (m // nb) * nb + my_slot
        return remote(
            meta_ref, meta_all.at[m // nb, :, block_of(my_slot)], meta_s.at[m], meta_r.at[slot],
            {"ep": to},
        )

    def arrival(m):
        return remote(
            meta_ref, meta_all.at[m // nb, :, block_of(lax.rem(m, nb))], meta_s.at[m],
            meta_r.at[m], {"ep": lax.rem(me + 1, nep)},
        )

    def start(m, carry):
        @pl.when(m != my_slot)
        def _():
            give(m).start()

        return carry

    def finish(m, carry):
        @pl.when(m != my_slot)
        def _():
            arrival(m).wait_recv()

        return carry

    def sent(m, carry):
        @pl.when(m != my_slot)
        def _():
            give(m).wait_send()

        return carry

    lax.fori_loop(0, nep, start, 0)
    meta_all[0, :, block_of(my_slot)] = meta_ref[...]
    lax.fori_loop(0, nep, finish, 0)
    chips = nep // 2
    loads = jnp.zeros((nq * chips, span), jnp.float32)
    line = lax.broadcasted_iota(jnp.int32, (nq * chips, span), 0)
    for q in range(nq):
        ids = meta_all[q, :top, :]
        all_ref[q] = meta_all[q]
        for c in range(chips):
            here = jnp.logical_and(ids >= c * 2 * local, ids < (c + 1) * 2 * local)
            row = jnp.sum(here.astype(jnp.float32), axis=0, keepdims=True)
            loads = jnp.where(line == q * chips + c, row, loads)
    top_load = jnp.max(jnp.sum(loads, axis=1, keepdims=True))
    size = jnp.int32(0)
    for limit in limits:
        size += (top_load > float(limit)).astype(jnp.int32)
    size_ref[0] = size
    lax.fori_loop(0, nep, sent, 0)


def layer_kernel(
    nep, n, local, top, nq, full, half,
    tok_ref, meta_all, gw_hbm, uw_hbm, dw_hbm,
    out_ref,
    gu, dw, tok_all, place, gate, ends,
    xbuf, own, res, ra, rb, ha, hb, sp_out, sp_in, hs_in, acc, total_out, out_send, out_recv,
    gu_sem, dw_sem, tok_s, tok_r,
    ra_s, ra_r, rb_s, rb_r, ha_s, ha_r, hb_s, hb_r, sp_s, sp_r, hs_s, hs_r, out_s, out_r,
):
    me = lax.axis_index("ep")
    z = lax.axis_index("tp")
    spill = full - half
    low_row = half - spill
    partner = me + 1 - 2 * lax.rem(me, 2)
    rows = tok_ref.shape[0]
    nb = nep // nq
    span = nb * rows
    ng = gu.shape[0]
    pair = ng // dw.shape[0]
    late = pair if ng > pair else 0
    chunks = nq * ng
    bf16, f32 = jnp.bfloat16, jnp.float32
    zl = lax.rem(z + n - 1, n)
    zr = lax.rem(z + 1, n)
    my_group = me // nb
    my_slot = lax.rem(me, nb)

    def gate_copy(g):
        return pltpu.make_async_copy(
            gw_hbm.at[:, :, pl.ds(g * LANES, LANES)],
            gu.at[g, :, :, pl.ds(0, LANES)], gu_sem.at[0, g],
        )

    def up_copy(g):
        return pltpu.make_async_copy(
            uw_hbm.at[:, :, pl.ds(g * LANES, LANES)],
            gu.at[g, :, :, pl.ds(LANES, LANES)], gu_sem.at[1, g],
        )

    def down_copy(i):
        return pltpu.make_async_copy(
            dw_hbm.at[:, :, pl.ds(i * pair * LANES, pair * LANES)], dw.at[i], dw_sem.at[i]
        )

    for g in range(ng):
        gate_copy((g + late) % ng).start()
        up_copy((g + late) % ng).start()
    for i in range(ng // pair):
        down_copy(i).start()

    barrier = pltpu.get_barrier_semaphore()

    def greet(j, carry):
        pl.semaphore_signal(
            barrier, inc=1, device_id={"ep": lax.rem(me + j, nep)}, device_id_type=MESH
        )
        return carry

    lax.fori_loop(1, nep, greet, 0)

    @pl.when(z > 0)
    def _():
        pl.semaphore_signal(barrier, inc=1, device_id={"tp": zl}, device_id_type=MESH)

    @pl.when(z < n - 1)
    def _():
        pl.semaphore_signal(barrier, inc=1, device_id={"tp": zr}, device_id_type=MESH)

    sides = (z > 0).astype(jnp.int32) + (z < n - 1).astype(jnp.int32)

    def block_of(i):
        return pl.ds(pl.multiple_of(i * rows, rows), rows)

    def tok_copy(m):
        to = lax.rem(my_group - m // nb + nq, nq) * nb + lax.rem(m, nb)
        slot = (m // nb) * nb + my_slot
        return remote(
            tok_ref, tok_all.at[m // nb, block_of(my_slot), :], tok_s.at[m], tok_r.at[slot],
            {"ep": to},
        )

    def tok_arrival(m):
        return remote(
            tok_ref, tok_all.at[m // nb, block_of(lax.rem(m, nb)), :], tok_s.at[m], tok_r.at[m],
            {"ep": lax.rem(me + 1, nep)},
        )

    def out_copy(m):
        to = lax.rem(my_group + m // nb, nq) * nb + lax.rem(m, nb)
        return remote(
            out_send.at[m // nb, block_of(lax.rem(m, nb)), :], out_recv.at[me],
            out_s.at[m], out_r.at[me], {"ep": to},
        )

    def out_arrival(j):
        source = lax.rem(me + j, nep)
        return source, remote(
            out_send.at[0, block_of(0), :], out_recv.at[source],
            out_s.at[0], out_r.at[source], {"ep": source},
        )

    def ra_copy(k):
        return remote(ra.at[k], ra.at[k], ra_s.at[k], ra_r.at[k], {"tp": zl})

    def rb_copy(k):
        return remote(rb.at[k], rb.at[k], rb_s.at[k], rb_r.at[k], {"tp": zr})

    def ha_copy(k):
        return remote(ha.at[k], ha.at[k], ha_s.at[k], ha_r.at[k], {"tp": zr})

    def hb_copy(k):
        return remote(hb.at[k], hb.at[k], hb_s.at[k], hb_r.at[k], {"tp": zl})

    before = (
        lax.broadcasted_iota(jnp.int32, (span, span), 0)
        < lax.broadcasted_iota(jnp.int32, (span, span), 1)
    ).astype(bf16)

    def row_ids(d, lanes):
        r = lax.broadcasted_iota(jnp.int32, (full, lanes), 0)
        mine = 2 * r + d
        lent = 2 * full - 1 - d - 2 * (r - half)
        return jnp.where(r < half, mine, lent).astype(f32)
    sub_id = lax.broadcasted_iota(jnp.int32, (16, span), 0)

    def arrive(q):
        def one(i, carry):
            m = q * nb + i

            @pl.when(m != my_slot)
            def _():
                tok_arrival(m).wait_recv()

            return carry

        lax.fori_loop(0, nb, one, 0)

    def prepare(q):
        ids = meta_all[q, :top, :]
        fixed = meta_all[q, top:, :]
        chosen, wide = [], jnp.zeros((16, span), f32)
        for e in range(local):
            named = ids == me * local + e
            row = jnp.sum(named.astype(f32), axis=0, keepdims=True)
            weight = jnp.sum(jnp.where(named, fixed, 0), axis=0, keepdims=True)
            gate[q, e:e + 1, :] = weight.astype(f32) * (1.0 / 65536.0)
            wide = jnp.where(sub_id == e, row, wide)
            chosen.append(row)
        earlier = jnp.dot(wide.astype(bf16), before, preferred_element_type=f32)
        base = jnp.zeros((1, 1), f32)
        for e in range(local):
            place[q, e:e + 1, :] = jnp.where(
                chosen[e] > 0.5, base + earlier[e:e + 1, :], -1.0
            )
            base = base + jnp.sum(chosen[e], axis=1, keepdims=True)
            ends[q, e:e + 1, :] = jnp.broadcast_to(base, (1, LANES))

    prepare(0)
    pl.semaphore_wait(barrier, nep - 1 + sides)

    def send_tokens(m, carry):
        @pl.when(m != my_slot)
        def _():
            tok_copy(m).start()

        return carry

    lax.fori_loop(0, nep, send_tokens, 0)
    tok_all[0, block_of(my_slot), :] = tok_ref[...]

    def clear(j, carry):
        acc[j] = jnp.zeros(acc.shape[1:], acc.dtype)
        return carry

    lax.fori_loop(0, nq, clear, 0)

    def inside(k):
        return jnp.logical_and(k >= 0, k < chunks)

    def decode(k):
        c = lax.rem(k + late, chunks)
        return c // ng, lax.rem(c, ng)

    def spot(q, g):
        return lax.rem(q * ng + g + chunks - late, chunks)

    def lend_copy(k, d):
        i = d * chunks + k
        return remote(sp_out.at[i], sp_in.at[i], sp_s.at[i], sp_r.at[i], {"ep": partner})

    def back_copy(k, d, hidden):
        i = d * chunks + k
        return remote(
            hidden.at[k, pl.ds(low_row, spill), :], hs_in.at[i], hs_s.at[i], hs_r.at[i],
            {"ep": partner},
        )

    def product_stage(k, d):
        @pl.when(inside(k))
        def _():
            q, g = decode(k)

            @pl.when(jnp.logical_or(k == 0, g == 0))
            def _():
                ids = row_ids(d, span)
                for e in range(local):
                    pick = ids == place[q, e:e + 1, :]
                    xbuf[d, e] = jnp.dot(
                        pick.astype(bf16), tok_all[q], preferred_element_type=f32
                    ).astype(bf16)

            total = jnp.dot(xbuf[d, 0], gu[g, 0], preferred_element_type=f32)
            for e in range(1, local):
                total += jnp.dot(xbuf[d, e], gu[g, e], preferred_element_type=f32)
            own[d, lax.rem(k, LEAD + 1)] = total[:half]
            if spill:
                sp_out[d * chunks + k] = total[half:]
                lend_copy(k, d).start()

    def chain_stage(k, d, buf, copy, has_source, is_last, hidden):
        @pl.when(inside(k))
        def _():
            mine = own.at[d, lax.rem(k, LEAD + 1)]
            if spill:
                lend_copy(k, d).wait_recv()
                mine[low_row:, :] += sp_in[d * chunks + k]

            @pl.when(has_source)
            def _():
                copy(k).wait_recv()

            @pl.when(jnp.logical_and(has_source, jnp.logical_not(is_last)))
            def _():
                buf[k] = (mine[...] + buf[k].astype(f32)).astype(bf16)
                copy(k).start()

            @pl.when(jnp.logical_not(has_source))
            def _():
                buf[k] = mine[...].astype(bf16)
                copy(k).start()

            @pl.when(is_last)
            def _():
                v = mine[:, :LANES] + buf[k, :, :LANES].astype(f32)
                w = mine[:, LANES:] + buf[k, :, LANES:].astype(f32)
                hidden[k] = (v / (1.0 + jnp.exp(-v)) * w).astype(bf16)

    def hidden_stage(k, d, hidden, copy, has_source, is_last):
        @pl.when(inside(k))
        def _():
            @pl.when(has_source)
            def _():
                copy(k).wait_recv()

            @pl.when(jnp.logical_not(is_last))
            def _():
                copy(k).start()

            if spill:
                back_copy(k, d, hidden).start()

    def down_stage(k, d, hidden):
        @pl.when(inside(k))
        def _():
            if spill:
                back_copy(k, d, hidden).wait_recv()
            q, g = decode(k)
            home = (q == 0).astype(jnp.int32)

            @pl.when(lax.rem(g, pair) == pair - 1)
            def _():
                parts = [spot(q, g - pair + 1 + i) for i in range(pair)]
                units = jnp.concatenate([hidden[i] for i in parts], axis=1)
                if spill:
                    lent = jnp.concatenate([hs_in[d * chunks + i] for i in parts], axis=1)
                    units = jnp.concatenate([units, lent], axis=0)
                at = row_ids(d, LANES)
                start = jnp.zeros((1, LANES), f32)
                result = jnp.zeros((dw.shape[2], full), f32)
                for e in range(local):
                    end = ends[q, e:e + 1, :]
                    mine = jnp.logical_and(at >= start, at < end).astype(f32).astype(bf16)
                    start = end
                    result += lax.dot_general(
                        dw[g // pair, e], units * jnp.concatenate([mine] * pair, axis=1),
                        (((1,), (1,)), ((), ())), preferred_element_type=f32,
                    )
                first = jnp.logical_or(
                    k == pair - 1, jnp.logical_and(q > 0, g == pair - 1)
                )

                @pl.when(first)
                def _():
                    res[d, home] = result

                @pl.when(jnp.logical_not(first))
                def _():
                    res[d, home] += result

            @pl.when(complete(k))
            def _():
                ids = row_ids(d, span)
                top_part = jnp.zeros((full, span), f32)
                for e in range(local):
                    pick = ids == place[q, e:e + 1, :]
                    top_part = jnp.where(pick, gate[q, e:e + 1, :], top_part)
                coarse = top_part.astype(bf16)
                fine = (top_part - coarse.astype(f32)).astype(bf16)
                value = res[d, home]
                high = value.astype(bf16)
                low = (value - high.astype(f32)).astype(bf16)
                acc[q] += jnp.dot(
                    jnp.concatenate([high, high, low], axis=1),
                    jnp.concatenate([coarse, fine, coarse], axis=0),
                    preferred_element_type=f32,
                )

    def complete(k):
        q, g = decode(k)
        if late == 0:
            return g == ng - 1
        return jnp.logical_or(k == chunks - 1, jnp.logical_and(q > 0, g == ng - 1))

    turn = SKEW * (n - 1)
    from_right = SKEW * (n - 1 - z)
    from_left = SKEW * z
    lead = jnp.minimum(from_left, from_right)

    def step(t, carry):
        k_first = t - lead
        q_first, g_first = decode(k_first)

        @pl.when(jnp.logical_and(inside(k_first), jnp.logical_and(q_first > 0, g_first == 0)))
        def _():
            prepare(q_first)
            arrive(q_first)

        @pl.when(jnp.logical_and(inside(k_first), k_first < ng))
        def _():
            gate_copy(g_first).wait()
            up_copy(g_first).wait()

        @pl.when(t == LEAD + LATE + turn + lead + pair - 1)
        def _():
            for i in range(ng // pair):
                down_copy(i).wait()

        back = t - LEAD - turn
        chain_stage(t - LEAD - from_right, 0, ra, ra_copy, z < n - 1, z == 0, ha)
        chain_stage(t - LEAD - from_left, 1, rb, rb_copy, z > 0, z == n - 1, hb)
        hidden_stage(back - from_left, 0, ha, ha_copy, z > 0, z == n - 1)
        hidden_stage(back - from_right, 1, hb, hb_copy, z < n - 1, z == 0)
        product_stage(t - from_right, 0)
        product_stage(t - from_left, 1)
        down_stage(back - LATE - from_left, 0, ha)
        down_stage(back - LATE - from_right, 1, hb)
        k_done = back - LATE - jnp.maximum(from_left, from_right)

        @pl.when(jnp.logical_and(inside(k_done), complete(k_done)))
        def _():
            q, _ = decode(k_done)
            out_send[q] = acc[q].T.astype(bf16)

            def give(i, carry):
                m = q * nb + i

                @pl.when(m != my_slot)
                def _():
                    out_copy(m).start()

                return carry

            lax.fori_loop(0, nb, give, 0)

        return carry

    arrive(0)
    lax.fori_loop(0, chunks + 2 * turn + LEAD + LATE, step, 0)

    def finish_chunk(k, carry):
        if spill:
            lend_copy(k, 0).wait_send()
            lend_copy(k, 1).wait_send()
            back_copy(k, 0, ha).wait_send()
            back_copy(k, 1, hb).wait_send()

        @pl.when(z > 0)
        def _():
            ra_copy(k).wait_send()
            hb_copy(k).wait_send()

        @pl.when(z < n - 1)
        def _():
            rb_copy(k).wait_send()
            ha_copy(k).wait_send()

        return carry

    lax.fori_loop(0, chunks, finish_chunk, 0)

    def finish_send(m, carry):
        @pl.when(m != my_slot)
        def _():
            tok_copy(m).wait_send()
            out_copy(m).wait_send()

        return carry

    lax.fori_loop(0, nep, finish_send, 0)
    total_out[...] = acc[0, :, block_of(my_slot)].T

    def finish_block(j, carry):
        source, copy = out_arrival(j)
        copy.wait_recv()
        total_out[...] += out_recv[source].astype(f32)
        return carry

    lax.fori_loop(1, nep, finish_block, 0)
    out_ref[...] = total_out[...].astype(bf16)


def count_call(nep, nq, local, limits, routing, gate_fixed):
    rows, top = routing.shape
    depth = 2 * top
    nb = nep // nq
    dma = pltpu.SemaphoreType.DMA
    vmem = pl.BlockSpec(memory_space=pltpu.VMEM)
    shape = (nq, depth, nb * rows)
    return pl.pallas_call(
        functools.partial(count_kernel, nep, nq, local, top, limits),
        out_shape=(
            jax.ShapeDtypeStruct(shape, jnp.int32), jax.ShapeDtypeStruct((1,), jnp.int32)
        ),
        in_specs=[vmem, vmem],
        out_specs=(vmem, pl.BlockSpec(memory_space=pltpu.SMEM)),
        scratch_shapes=[
            pltpu.VMEM((depth, rows), jnp.int32), pltpu.VMEM(shape, jnp.int32),
            dma((nep,)), dma((nep,)),
        ],
        compiler_params=pltpu.CompilerParams(collective_id=0, has_side_effects=True),
    )(routing.T, gate_fixed.T)


def layer_call(nep, n, nq, top, full, half, number, tokens, meta_all, gate_weight, up_weight, down_weight):
    local, share, width = gate_weight.shape
    rows = tokens.shape[0]
    nb = nep // nq
    ng = width // LANES
    chunks = nq * ng
    pair = 2 if ng % 2 == 0 else 1
    spill = max(full - half, 16)
    lent = 2 * chunks if half < full else 1
    bf16, f32 = jnp.bfloat16, jnp.float32
    dma = pltpu.SemaphoreType.DMA
    vmem = pl.BlockSpec(memory_space=pltpu.VMEM)
    hbm = pl.BlockSpec(memory_space=pl.ANY)
    return pl.pallas_call(
        functools.partial(layer_kernel, nep, n, local, top, nq, full, half),
        out_shape=jax.ShapeDtypeStruct((rows, share), bf16),
        in_specs=[vmem, vmem, hbm, hbm, hbm],
        out_specs=vmem,
        scratch_shapes=[
            pltpu.VMEM((ng, local, share, 2 * LANES), bf16),
            pltpu.VMEM((ng // pair, local, share, pair * LANES), bf16),
            pltpu.VMEM((nq, nb * rows, share), bf16),
            pltpu.VMEM((nq, 8, nb * rows), f32),
            pltpu.VMEM((nq, 8, nb * rows), f32),
            pltpu.VMEM((nq, 8, LANES), f32),
            pltpu.VMEM((2, local, full, share), bf16),
            pltpu.VMEM((2, LEAD + 1, half, 2 * LANES), f32),
            pltpu.VMEM((2, 2, share, full), f32),
            pltpu.VMEM((chunks, half, 2 * LANES), bf16),
            pltpu.VMEM((chunks, half, 2 * LANES), bf16),
            pltpu.VMEM((chunks, half, LANES), bf16),
            pltpu.VMEM((chunks, half, LANES), bf16),
            pltpu.VMEM((lent, spill, 2 * LANES), f32),
            pltpu.VMEM((lent, spill, 2 * LANES), f32),
            pltpu.VMEM((lent, spill, LANES), bf16),
            pltpu.VMEM((nq, share, nb * rows), f32),
            pltpu.VMEM((rows, share), f32),
            pltpu.VMEM((nq, nb * rows, share), bf16),
            pltpu.VMEM((nep, rows, share), bf16),
            dma((2, ng)), dma((ng // pair,)),
            dma((nep,)), dma((nep,)),
            dma((chunks,)), dma((chunks,)), dma((chunks,)), dma((chunks,)),
            dma((chunks,)), dma((chunks,)), dma((chunks,)), dma((chunks,)),
            dma((lent,)), dma((lent,)), dma((lent,)), dma((lent,)),
            dma((nep,)), dma((nep,)),
        ],
        compiler_params=pltpu.CompilerParams(
            collective_id=number, has_side_effects=True, vmem_limit_bytes=60 * 1024 * 1024
        ),
    )(tokens, meta_all, gate_weight, up_weight, down_weight)


def on_device(nep, n, tokens, routing, gate_fixed, gate_weight, up_weight, down_weight):
    local = gate_weight.shape[0]
    rows, top = routing.shape
    cap = max(2, rows * top * 2 // (local * nep))
    nq = min(GROUPS, nep)
    full = nep // nq * local * cap // 2
    halves = [h for h in (full * s // 32 for s in SIZES) if h % 8 == 0] + [full]
    meta_all, size = count_call(
        nep, nq, local, [4 * h for h in halves[:-1]], routing, gate_fixed
    )
    calls = [
        functools.partial(layer_call, nep, n, nq, top, full, h, i + 1)
        for i, h in enumerate(halves)
    ]
    return lax.switch(
        size[0], calls, tokens, meta_all, gate_weight, up_weight, down_weight
    )


def solution(mesh):
    in_specs = (
        P("ep", "tp"),
        P("ep", None),
        P("ep", None),
        P("ep", "tp", None),
        P("ep", "tp", None),
        P("ep", "tp", None),
    )
    body = functools.partial(on_device, mesh.shape["ep"], mesh.shape["tp"])
    return jax.shard_map(
        body, mesh=mesh, in_specs=in_specs, out_specs=P("ep", "tp"), check_vma=False
    )
```

```python
import functools

import jax
import jax.numpy as jnp
from jax import lax
from jax.experimental import pallas as pl
from jax.experimental.pallas import tpu as pltpu
from jax.sharding import PartitionSpec as P

MESH = pl.DeviceIdType.MESH
SKEW = 4
LEAD = 3
LATE = 1
GROUPS = 4
LANES = 128
SIZES = (18, 19, 20, 21, 22)


def remote(src, dst, s, r, device):
    return pltpu.make_async_remote_copy(
        src_ref=src, dst_ref=dst, send_sem=s, recv_sem=r,
        device_id=device, device_id_type=MESH,
    )


def differ(a, b):
    return lax.rem(a // 2 + b // 2, 2) * 2 + lax.rem(a + b, 2)


def group_at(mine, q):
    return differ(mine, differ(q, q // 2))


def count_kernel(
    nep, nq, local, top, limits,
    ids_ref, gate_ref, all_ref, size_ref, meta_ref, meta_all, meta_s, meta_r,
):
    me = lax.axis_index("ep")
    rows = meta_ref.shape[1]
    nb = nep // nq
    span = nb * rows
    my_group = me // nb
    my_slot = lax.rem(me, nb)
    barrier = pltpu.get_barrier_semaphore()

    def greet(j, carry):
        pl.semaphore_signal(
            barrier, inc=1, device_id={"ep": lax.rem(me + j, nep)}, device_id_type=MESH
        )
        return carry

    lax.fori_loop(1, nep, greet, 0)
    meta_ref[:top] = ids_ref[...]
    meta_ref[top:] = gate_ref[...]
    pl.semaphore_wait(barrier, nep - 1)

    def block_of(i):
        return pl.ds(pl.multiple_of(i * rows, rows), rows)

    def give(m):
        to = group_at(my_group, m // nb) * nb + lax.rem(m, nb)
        slot = (m // nb) * nb + my_slot
        return remote(
            meta_ref, meta_all.at[m // nb, :, block_of(my_slot)], meta_s.at[m], meta_r.at[slot],
            {"ep": to},
        )

    def arrival(m):
        return remote(
            meta_ref, meta_all.at[m // nb, :, block_of(lax.rem(m, nb))], meta_s.at[m],
            meta_r.at[m], {"ep": lax.rem(me + 1, nep)},
        )

    def start(m, carry):
        @pl.when(m != my_slot)
        def _():
            give(m).start()

        return carry

    def finish(m, carry):
        @pl.when(m != my_slot)
        def _():
            arrival(m).wait_recv()

        return carry

    def sent(m, carry):
        @pl.when(m != my_slot)
        def _():
            give(m).wait_send()

        return carry

    lax.fori_loop(0, nep, start, 0)
    meta_all[0, :, block_of(my_slot)] = meta_ref[...]
    lax.fori_loop(0, nep, finish, 0)
    chips = nep // 2
    loads = jnp.zeros((nq * chips, span), jnp.float32)
    line = lax.broadcasted_iota(jnp.int32, (nq * chips, span), 0)
    for q in range(nq):
        ids = meta_all[q, :top, :]
        all_ref[q] = meta_all[q]
        for c in range(chips):
            here = jnp.logical_and(ids >= c * 2 * local, ids < (c + 1) * 2 * local)
            row = jnp.sum(here.astype(jnp.float32), axis=0, keepdims=True)
            loads = jnp.where(line == q * chips + c, row, loads)
    top_load = jnp.max(jnp.sum(loads, axis=1, keepdims=True))
    size = jnp.int32(0)
    for limit in limits:
        size += (top_load > float(limit)).astype(jnp.int32)
    size_ref[0] = size
    lax.fori_loop(0, nep, sent, 0)


def layer_kernel(
    nep, n, local, top, nq, full, half,
    tok_ref, meta_all, gw_hbm, uw_hbm, dw_hbm,
    out_ref,
    gu, dw, tok_all, place, gate, ends,
    xbuf, own, res, ra, rb, ha, hb, sp_out, sp_in, hs_in, acc, total_out, out_send, out_recv,
    gu_sem, dw_sem, tok_s, tok_r,
    ra_s, ra_r, rb_s, rb_r, ha_s, ha_r, hb_s, hb_r, sp_s, sp_r, hs_s, hs_r, out_s, out_r,
):
    me = lax.axis_index("ep")
    z = lax.axis_index("tp")
    spill = full - half
    low_row = half - spill
    partner = me + 1 - 2 * lax.rem(me, 2)
    rows = tok_ref.shape[0]
    nb = nep // nq
    span = nb * rows
    ng = gu.shape[0]
    pair = ng // dw.shape[0]
    late = pair if ng > pair else 0
    chunks = nq * ng
    bf16, f32 = jnp.bfloat16, jnp.float32
    zl = lax.rem(z + n - 1, n)
    zr = lax.rem(z + 1, n)
    my_group = me // nb
    my_slot = lax.rem(me, nb)

    def gate_copy(g):
        return pltpu.make_async_copy(
            gw_hbm.at[:, :, pl.ds(g * LANES, LANES)],
            gu.at[g, :, :, pl.ds(0, LANES)], gu_sem.at[0, g],
        )

    def up_copy(g):
        return pltpu.make_async_copy(
            uw_hbm.at[:, :, pl.ds(g * LANES, LANES)],
            gu.at[g, :, :, pl.ds(LANES, LANES)], gu_sem.at[1, g],
        )

    def down_copy(i):
        return pltpu.make_async_copy(
            dw_hbm.at[:, :, pl.ds(i * pair * LANES, pair * LANES)], dw.at[i], dw_sem.at[i]
        )

    for g in range(ng):
        gate_copy((g + late) % ng).start()
        up_copy((g + late) % ng).start()
    for i in range(ng // pair):
        down_copy(i).start()

    barrier = pltpu.get_barrier_semaphore()

    def greet(j, carry):
        pl.semaphore_signal(
            barrier, inc=1, device_id={"ep": lax.rem(me + j, nep)}, device_id_type=MESH
        )
        return carry

    lax.fori_loop(1, nep, greet, 0)

    @pl.when(z > 0)
    def _():
        pl.semaphore_signal(barrier, inc=1, device_id={"tp": zl}, device_id_type=MESH)

    @pl.when(z < n - 1)
    def _():
        pl.semaphore_signal(barrier, inc=1, device_id={"tp": zr}, device_id_type=MESH)

    sides = (z > 0).astype(jnp.int32) + (z < n - 1).astype(jnp.int32)

    def block_of(i):
        return pl.ds(pl.multiple_of(i * rows, rows), rows)

    def tok_copy(m):
        to = group_at(my_group, m // nb) * nb + lax.rem(m, nb)
        slot = (m // nb) * nb + my_slot
        return remote(
            tok_ref, tok_all.at[m // nb, block_of(my_slot), :], tok_s.at[m], tok_r.at[slot],
            {"ep": to},
        )

    def tok_arrival(m):
        return remote(
            tok_ref, tok_all.at[m // nb, block_of(lax.rem(m, nb)), :], tok_s.at[m], tok_r.at[m],
            {"ep": lax.rem(me + 1, nep)},
        )

    def out_copy(m):
        to = group_at(my_group, m // nb) * nb + lax.rem(m, nb)
        return remote(
            out_send.at[m // nb, block_of(lax.rem(m, nb)), :], out_recv.at[me],
            out_s.at[m], out_r.at[me], {"ep": to},
        )

    def out_arrival(j):
        source = lax.rem(me + j, nep)
        return source, remote(
            out_send.at[0, block_of(0), :], out_recv.at[source],
            out_s.at[0], out_r.at[source], {"ep": source},
        )

    def ra_copy(k):
        return remote(ra.at[k], ra.at[k], ra_s.at[k], ra_r.at[k], {"tp": zl})

    def rb_copy(k):
        return remote(rb.at[k], rb.at[k], rb_s.at[k], rb_r.at[k], {"tp": zr})

    def ha_copy(k):
        return remote(ha.at[k], ha.at[k], ha_s.at[k], ha_r.at[k], {"tp": zr})

    def hb_copy(k):
        return remote(hb.at[k], hb.at[k], hb_s.at[k], hb_r.at[k], {"tp": zl})

    before = (
        lax.broadcasted_iota(jnp.int32, (span, span), 0)
        < lax.broadcasted_iota(jnp.int32, (span, span), 1)
    ).astype(bf16)

    def row_ids(d, lanes):
        r = lax.broadcasted_iota(jnp.int32, (full, lanes), 0)
        mine = 2 * r + d
        lent = 2 * full - 1 - d - 2 * (r - half)
        return jnp.where(r < half, mine, lent).astype(f32)
    sub_id = lax.broadcasted_iota(jnp.int32, (16, span), 0)

    def arrive(q):
        def one(i, carry):
            m = q * nb + i

            @pl.when(m != my_slot)
            def _():
                tok_arrival(m).wait_recv()

            return carry

        lax.fori_loop(0, nb, one, 0)

    def prepare(q):
        ids = meta_all[q, :top, :]
        fixed = meta_all[q, top:, :]
        chosen, wide = [], jnp.zeros((16, span), f32)
        for e in range(local):
            named = ids == me * local + e
            row = jnp.sum(named.astype(f32), axis=0, keepdims=True)
            weight = jnp.sum(jnp.where(named, fixed, 0), axis=0, keepdims=True)
            gate[q, e:e + 1, :] = weight.astype(f32) * (1.0 / 65536.0)
            wide = jnp.where(sub_id == e, row, wide)
            chosen.append(row)
        earlier = jnp.dot(wide.astype(bf16), before, preferred_element_type=f32)
        base = jnp.zeros((1, 1), f32)
        for e in range(local):
            place[q, e:e + 1, :] = jnp.where(
                chosen[e] > 0.5, base + earlier[e:e + 1, :], -1.0
            )
            base = base + jnp.sum(chosen[e], axis=1, keepdims=True)
            ends[q, e:e + 1, :] = jnp.broadcast_to(base, (1, LANES))

    prepare(0)
    pl.semaphore_wait(barrier, nep - 1 + sides)

    def send_tokens(m, carry):
        @pl.when(m != my_slot)
        def _():
            tok_copy(m).start()

        return carry

    lax.fori_loop(0, nep, send_tokens, 0)
    tok_all[0, block_of(my_slot), :] = tok_ref[...]

    def clear(j, carry):
        acc[j] = jnp.zeros(acc.shape[1:], acc.dtype)
        return carry

    lax.fori_loop(0, nq, clear, 0)

    def inside(u, part):
        fits = jnp.logical_and(u >= 0, u < 2 * chunks)
        return fits if part is None else jnp.logical_and(fits, lax.rem(u, 2) == part)

    def decode(k):
        c = lax.rem(k + late, chunks)
        return c // ng, lax.rem(c, ng)

    def spot(q, g):
        return lax.rem(q * ng + g + chunks - late, chunks)

    def lend_copy(k, d):
        i = d * chunks + k
        return remote(sp_out.at[i], sp_in.at[i], sp_s.at[i], sp_r.at[i], {"ep": partner})

    def back_copy(k, d, hidden):
        i = d * chunks + k
        return remote(
            hidden.at[k, pl.ds(low_row, spill), :], hs_in.at[i], hs_s.at[i], hs_r.at[i],
            {"ep": partner},
        )

    def product_stage(u, d):
        @pl.when(inside(u, 0))
        def _():
            k = u // 2
            q, g = decode(k)

            @pl.when(jnp.logical_or(k == 0, g == 0))
            def _():
                ids = row_ids(d, span)
                for e in range(local):
                    pick = ids == place[q, e:e + 1, :]
                    xbuf[d, e] = jnp.dot(
                        pick.astype(bf16), tok_all[q], preferred_element_type=f32
                    ).astype(bf16)

            total = jnp.dot(xbuf[d, 0], gu[g, 0], preferred_element_type=f32)
            for e in range(1, local):
                total += jnp.dot(xbuf[d, e], gu[g, e], preferred_element_type=f32)
            for p in range(2):
                own[d, lax.rem(k, 3), p] = total[:half, p * LANES:(p + 1) * LANES]
            if spill:
                sp_out[d * chunks + k] = total[half:]
                lend_copy(k, d).start()

    def chain_stage(u, d, buf, copy, has_source, is_last, hidden):
        @pl.when(inside(u, None))
        def _():
            k = u // 2
            p = lax.rem(u, 2)
            mine = own.at[d, lax.rem(k, 3), p]
            if spill:
                @pl.when(p == 0)
                def _():
                    lend_copy(k, d).wait_recv()
                    for i in range(2):
                        own[d, lax.rem(k, 3), i, low_row:, :] += sp_in[
                            d * chunks + k, :, i * LANES:(i + 1) * LANES
                        ]

            @pl.when(has_source)
            def _():
                copy(u).wait_recv()

            @pl.when(jnp.logical_and(has_source, jnp.logical_not(is_last)))
            def _():
                buf[u] = (mine[...] + buf[u].astype(f32)).astype(bf16)
                copy(u).start()

            @pl.when(jnp.logical_not(has_source))
            def _():
                buf[u] = mine[...].astype(bf16)
                copy(u).start()

            @pl.when(jnp.logical_and(is_last, p == 1))
            def _():
                v = own[d, lax.rem(k, 3), 0] + buf[u - 1].astype(f32)
                w = mine[...] + buf[u].astype(f32)
                hidden[k] = (v / (1.0 + jnp.exp(-v)) * w).astype(bf16)

    def hidden_stage(u, d, hidden, copy, has_source, is_last):
        @pl.when(inside(u, 1))
        def _():
            k = u // 2

            @pl.when(has_source)
            def _():
                copy(k).wait_recv()

            @pl.when(jnp.logical_not(is_last))
            def _():
                copy(k).start()

            if spill:
                back_copy(k, d, hidden).start()

    def down_stage(u, d, hidden):
        @pl.when(inside(u, 1))
        def _():
            k = u // 2
            if spill:
                back_copy(k, d, hidden).wait_recv()
            q, g = decode(k)
            home = (q == 0).astype(jnp.int32)

            @pl.when(lax.rem(g, pair) == pair - 1)
            def _():
                parts = [spot(q, g - pair + 1 + i) for i in range(pair)]
                units = jnp.concatenate([hidden[i] for i in parts], axis=1)
                if spill:
                    lent = jnp.concatenate([hs_in[d * chunks + i] for i in parts], axis=1)
                    units = jnp.concatenate([units, lent], axis=0)
                at = row_ids(d, LANES)
                start = jnp.zeros((1, LANES), f32)
                result = jnp.zeros((dw.shape[2], full), f32)
                for e in range(local):
                    end = ends[q, e:e + 1, :]
                    mine = jnp.logical_and(at >= start, at < end).astype(f32).astype(bf16)
                    start = end
                    result += lax.dot_general(
                        dw[g // pair, e], units * jnp.concatenate([mine] * pair, axis=1),
                        (((1,), (1,)), ((), ())), preferred_element_type=f32,
                    )
                first = jnp.logical_or(
                    k == pair - 1, jnp.logical_and(q > 0, g == pair - 1)
                )

                @pl.when(first)
                def _():
                    res[d, home] = result

                @pl.when(jnp.logical_not(first))
                def _():
                    res[d, home] += result

            @pl.when(complete(k))
            def _():
                ids = row_ids(d, span)
                top_part = jnp.zeros((full, span), f32)
                for e in range(local):
                    pick = ids == place[q, e:e + 1, :]
                    top_part = jnp.where(pick, gate[q, e:e + 1, :], top_part)
                coarse = top_part.astype(bf16)
                fine = (top_part - coarse.astype(f32)).astype(bf16)
                value = res[d, home]
                high = value.astype(bf16)
                low = (value - high.astype(f32)).astype(bf16)
                acc[q] += jnp.dot(
                    jnp.concatenate([high, high, low], axis=1),
                    jnp.concatenate([coarse, fine, coarse], axis=0),
                    preferred_element_type=f32,
                )

    def complete(k):
        q, g = decode(k)
        if late == 0:
            return g == ng - 1
        return jnp.logical_or(k == chunks - 1, jnp.logical_and(q > 0, g == ng - 1))

    turn = SKEW * (n - 1)
    from_right = SKEW * (n - 1 - z)
    from_left = SKEW * z
    lead = jnp.minimum(from_left, from_right)

    def step(t, carry):
        u_first = t - lead
        k_first = u_first // 2
        q_first, g_first = decode(k_first)

        @pl.when(jnp.logical_and(inside(u_first, 0), jnp.logical_and(q_first > 0, g_first == 0)))
        def _():
            prepare(q_first)
            arrive(q_first)

        @pl.when(jnp.logical_and(inside(u_first, 0), k_first < ng))
        def _():
            gate_copy(g_first).wait()
            up_copy(g_first).wait()

        @pl.when(t == LEAD + LATE + turn + lead + 2 * pair - 1)
        def _():
            for i in range(ng // pair):
                down_copy(i).wait()

        back = t - LEAD - turn
        chain_stage(t - LEAD - from_right, 0, ra, ra_copy, z < n - 1, z == 0, ha)
        chain_stage(t - LEAD - from_left, 1, rb, rb_copy, z > 0, z == n - 1, hb)
        hidden_stage(back - from_left, 0, ha, ha_copy, z > 0, z == n - 1)
        hidden_stage(back - from_right, 1, hb, hb_copy, z < n - 1, z == 0)
        product_stage(t - from_right, 0)
        product_stage(t - from_left, 1)
        down_stage(back - LATE - from_left, 0, ha)
        down_stage(back - LATE - from_right, 1, hb)
        u_done = back - LATE - jnp.maximum(from_left, from_right)
        k_done = u_done // 2

        @pl.when(jnp.logical_and(inside(u_done, 1), complete(k_done)))
        def _():
            q, _ = decode(k_done)
            out_send[q] = acc[q].T.astype(bf16)

            def give(i, carry):
                m = q * nb + i

                @pl.when(m != my_slot)
                def _():
                    out_copy(m).start()

                return carry

            lax.fori_loop(0, nb, give, 0)

        return carry

    arrive(0)
    lax.fori_loop(0, 2 * chunks + 2 * turn + LEAD + LATE, step, 0)

    def finish_chunk(k, carry):
        if spill:
            lend_copy(k, 0).wait_send()
            lend_copy(k, 1).wait_send()
            back_copy(k, 0, ha).wait_send()
            back_copy(k, 1, hb).wait_send()

        @pl.when(z > 0)
        def _():
            ra_copy(2 * k).wait_send()
            ra_copy(2 * k + 1).wait_send()
            hb_copy(k).wait_send()

        @pl.when(z < n - 1)
        def _():
            rb_copy(2 * k).wait_send()
            rb_copy(2 * k + 1).wait_send()
            ha_copy(k).wait_send()

        return carry

    lax.fori_loop(0, chunks, finish_chunk, 0)

    def finish_send(m, carry):
        @pl.when(m != my_slot)
        def _():
            tok_copy(m).wait_send()
            out_copy(m).wait_send()

        return carry

    lax.fori_loop(0, nep, finish_send, 0)
    total_out[...] = acc[0, :, block_of(my_slot)].T

    def finish_block(j, carry):
        source, copy = out_arrival(j)
        copy.wait_recv()
        total_out[...] += out_recv[source].astype(f32)
        return carry

    lax.fori_loop(1, nep, finish_block, 0)
    out_ref[...] = total_out[...].astype(bf16)


def count_call(nep, nq, local, limits, routing, gate_fixed):
    rows, top = routing.shape
    depth = 2 * top
    nb = nep // nq
    dma = pltpu.SemaphoreType.DMA
    vmem = pl.BlockSpec(memory_space=pltpu.VMEM)
    shape = (nq, depth, nb * rows)
    return pl.pallas_call(
        functools.partial(count_kernel, nep, nq, local, top, limits),
        out_shape=(
            jax.ShapeDtypeStruct(shape, jnp.int32), jax.ShapeDtypeStruct((1,), jnp.int32)
        ),
        in_specs=[vmem, vmem],
        out_specs=(vmem, pl.BlockSpec(memory_space=pltpu.SMEM)),
        scratch_shapes=[
            pltpu.VMEM((depth, rows), jnp.int32), pltpu.VMEM(shape, jnp.int32),
            dma((nep,)), dma((nep,)),
        ],
        compiler_params=pltpu.CompilerParams(collective_id=0, has_side_effects=True),
    )(routing.T, gate_fixed.T)


def layer_call(nep, n, nq, top, full, half, number, tokens, meta_all, gate_weight, up_weight, down_weight):
    local, share, width = gate_weight.shape
    rows = tokens.shape[0]
    nb = nep // nq
    ng = width // LANES
    chunks = nq * ng
    pair = 2 if ng % 2 == 0 else 1
    spill = max(full - half, 16)
    lent = 2 * chunks if half < full else 1
    bf16, f32 = jnp.bfloat16, jnp.float32
    dma = pltpu.SemaphoreType.DMA
    vmem = pl.BlockSpec(memory_space=pltpu.VMEM)
    hbm = pl.BlockSpec(memory_space=pl.ANY)
    return pl.pallas_call(
        functools.partial(layer_kernel, nep, n, local, top, nq, full, half),
        out_shape=jax.ShapeDtypeStruct((rows, share), bf16),
        in_specs=[vmem, vmem, hbm, hbm, hbm],
        out_specs=vmem,
        scratch_shapes=[
            pltpu.VMEM((ng, local, share, 2 * LANES), bf16),
            pltpu.VMEM((ng // pair, local, share, pair * LANES), bf16),
            pltpu.VMEM((nq, nb * rows, share), bf16),
            pltpu.VMEM((nq, 8, nb * rows), f32),
            pltpu.VMEM((nq, 8, nb * rows), f32),
            pltpu.VMEM((nq, 8, LANES), f32),
            pltpu.VMEM((2, local, full, share), bf16),
            pltpu.VMEM((2, 3, 2, half, LANES), f32),
            pltpu.VMEM((2, 2, share, full), f32),
            pltpu.VMEM((2 * chunks, half, LANES), bf16),
            pltpu.VMEM((2 * chunks, half, LANES), bf16),
            pltpu.VMEM((chunks, half, LANES), bf16),
            pltpu.VMEM((chunks, half, LANES), bf16),
            pltpu.VMEM((lent, spill, 2 * LANES), f32),
            pltpu.VMEM((lent, spill, 2 * LANES), f32),
            pltpu.VMEM((lent, spill, LANES), bf16),
            pltpu.VMEM((nq, share, nb * rows), f32),
            pltpu.VMEM((rows, share), f32),
            pltpu.VMEM((nq, nb * rows, share), bf16),
            pltpu.VMEM((nep, rows, share), bf16),
            dma((2, ng)), dma((ng // pair,)),
            dma((nep,)), dma((nep,)),
            dma((2 * chunks,)), dma((2 * chunks,)), dma((2 * chunks,)), dma((2 * chunks,)),
            dma((chunks,)), dma((chunks,)), dma((chunks,)), dma((chunks,)),
            dma((lent,)), dma((lent,)), dma((lent,)), dma((lent,)),
            dma((nep,)), dma((nep,)),
        ],
        compiler_params=pltpu.CompilerParams(
            collective_id=number, has_side_effects=True, vmem_limit_bytes=60 * 1024 * 1024
        ),
    )(tokens, meta_all, gate_weight, up_weight, down_weight)


def on_device(nep, n, tokens, routing, gate_fixed, gate_weight, up_weight, down_weight):
    local = gate_weight.shape[0]
    rows, top = routing.shape
    cap = max(2, rows * top * 2 // (local * nep))
    nq = next(c for c in (GROUPS, 2, 1) if nep % c == 0)
    full = nep // nq * local * cap // 2
    halves = [h for h in (full * s // 32 for s in SIZES) if h % 8 == 0] + [full]
    meta_all, size = count_call(
        nep, nq, local, [4 * h for h in halves[:-1]], routing, gate_fixed
    )
    calls = [
        functools.partial(layer_call, nep, n, nq, top, full, h, i + 1)
        for i, h in enumerate(halves)
    ]
    return lax.switch(
        size[0], calls, tokens, meta_all, gate_weight, up_weight, down_weight
    )


def solution(mesh):
    in_specs = (
        P("ep", "tp"),
        P("ep", None),
        P("ep", None),
        P("ep", "tp", None),
        P("ep", "tp", None),
        P("ep", "tp", None),
    )
    body = functools.partial(on_device, mesh.shape["ep"], mesh.shape["tp"])
    return jax.shard_map(
        body, mesh=mesh, in_specs=in_specs, out_specs=P("ep", "tp"), check_vma=False
    )
```

```python
import functools

import jax
import jax.numpy as jnp
from jax import lax
from jax.experimental import pallas as pl
from jax.experimental.pallas import tpu as pltpu
from jax.sharding import PartitionSpec as P

MESH = pl.DeviceIdType.MESH
SKEW = 4
LEAD = 3
LATE = 1
GROUPS = 4
LANES = 128
SIZES = (18, 19, 20, 21, 22)


def remote(src, dst, s, r, device):
    return pltpu.make_async_remote_copy(
        src_ref=src, dst_ref=dst, send_sem=s, recv_sem=r,
        device_id=device, device_id_type=MESH,
    )


def differ(a, b):
    return lax.rem(a // 2 + b // 2, 2) * 2 + lax.rem(a + b, 2)


def group_at(mine, q):
    return differ(mine, differ(q, q // 2))


def count_kernel(
    nep, nq, local, top, limits,
    ids_ref, gate_ref, all_ref, size_ref, meta_ref, meta_all, meta_s, meta_r,
):
    me = lax.axis_index("ep")
    rows = meta_ref.shape[1]
    nb = nep // nq
    span = nb * rows
    my_group = me // nb
    my_slot = lax.rem(me, nb)
    barrier = pltpu.get_barrier_semaphore()

    def greet(j, carry):
        pl.semaphore_signal(
            barrier, inc=1, device_id={"ep": lax.rem(me + j, nep)}, device_id_type=MESH
        )
        return carry

    lax.fori_loop(1, nep, greet, 0)
    meta_ref[:top] = ids_ref[...]
    meta_ref[top:] = gate_ref[...]
    pl.semaphore_wait(barrier, nep - 1)

    def block_of(i):
        return pl.ds(pl.multiple_of(i * rows, rows), rows)

    def give(m):
        to = group_at(my_group, m // nb) * nb + lax.rem(m, nb)
        slot = (m // nb) * nb + my_slot
        return remote(
            meta_ref, meta_all.at[m // nb, :, block_of(my_slot)], meta_s.at[m], meta_r.at[slot],
            {"ep": to},
        )

    def arrival(m):
        return remote(
            meta_ref, meta_all.at[m // nb, :, block_of(lax.rem(m, nb))], meta_s.at[m],
            meta_r.at[m], {"ep": lax.rem(me + 1, nep)},
        )

    def start(m, carry):
        @pl.when(m != my_slot)
        def _():
            give(m).start()

        return carry

    def finish(m, carry):
        @pl.when(m != my_slot)
        def _():
            arrival(m).wait_recv()

        return carry

    def sent(m, carry):
        @pl.when(m != my_slot)
        def _():
            give(m).wait_send()

        return carry

    lax.fori_loop(0, nep, start, 0)
    meta_all[0, :, block_of(my_slot)] = meta_ref[...]
    lax.fori_loop(0, nep, finish, 0)
    chips = nep // 2
    loads = jnp.zeros((nq * chips, span), jnp.float32)
    line = lax.broadcasted_iota(jnp.int32, (nq * chips, span), 0)
    for q in range(nq):
        ids = meta_all[q, :top, :]
        all_ref[q] = meta_all[q]
        for c in range(chips):
            here = jnp.logical_and(ids >= c * 2 * local, ids < (c + 1) * 2 * local)
            row = jnp.sum(here.astype(jnp.float32), axis=0, keepdims=True)
            loads = jnp.where(line == q * chips + c, row, loads)
    top_load = jnp.max(jnp.sum(loads, axis=1, keepdims=True))
    size = jnp.int32(0)
    for limit in limits:
        size += (top_load > float(limit)).astype(jnp.int32)
    size_ref[0] = size
    lax.fori_loop(0, nep, sent, 0)


def layer_kernel(
    nep, n, local, top, nq, full, half,
    tok_ref, meta_all, gw_hbm, uw_hbm, dw_hbm,
    out_ref,
    gu, dw, tok_all, place, gate, ends,
    xbuf, own, res, ra, rb, ha, hb, sp_out, sp_in, hs_in, acc, total_out, out_send, out_recv,
    gu_sem, dw_sem, tok_s, tok_r,
    ra_s, ra_r, rb_s, rb_r, ha_s, ha_r, hb_s, hb_r, sp_s, sp_r, hs_s, hs_r, out_s, out_r,
):
    me = lax.axis_index("ep")
    z = lax.axis_index("tp")
    spill = full - half
    low_row = half - spill
    partner = me + 1 - 2 * lax.rem(me, 2)
    rows = tok_ref.shape[0]
    nb = nep // nq
    span = nb * rows
    ng = gu.shape[0]
    pair = ng // dw.shape[0]
    late = pair if ng > pair else 0
    chunks = nq * ng
    bf16, f32 = jnp.bfloat16, jnp.float32
    zl = lax.rem(z + n - 1, n)
    zr = lax.rem(z + 1, n)
    my_group = me // nb
    my_slot = lax.rem(me, nb)

    def gate_copy(g):
        return pltpu.make_async_copy(
            gw_hbm.at[:, :, pl.ds(g * LANES, LANES)],
            gu.at[g, :, :, pl.ds(0, LANES)], gu_sem.at[0, g],
        )

    def up_copy(g):
        return pltpu.make_async_copy(
            uw_hbm.at[:, :, pl.ds(g * LANES, LANES)],
            gu.at[g, :, :, pl.ds(LANES, LANES)], gu_sem.at[1, g],
        )

    def down_copy(i):
        return pltpu.make_async_copy(
            dw_hbm.at[:, :, pl.ds(i * pair * LANES, pair * LANES)], dw.at[i], dw_sem.at[i]
        )

    for g in range(ng):
        gate_copy((g + late) % ng).start()
        up_copy((g + late) % ng).start()
    for i in range(ng // pair):
        down_copy(i).start()

    barrier = pltpu.get_barrier_semaphore()

    def greet(j, carry):
        pl.semaphore_signal(
            barrier, inc=1, device_id={"ep": lax.rem(me + j, nep)}, device_id_type=MESH
        )
        return carry

    lax.fori_loop(1, nep, greet, 0)

    @pl.when(z > 0)
    def _():
        pl.semaphore_signal(barrier, inc=1, device_id={"tp": zl}, device_id_type=MESH)

    @pl.when(z < n - 1)
    def _():
        pl.semaphore_signal(barrier, inc=1, device_id={"tp": zr}, device_id_type=MESH)

    sides = (z > 0).astype(jnp.int32) + (z < n - 1).astype(jnp.int32)

    def block_of(i):
        return pl.ds(pl.multiple_of(i * rows, rows), rows)

    def tok_copy(m):
        to = group_at(my_group, m // nb) * nb + lax.rem(m, nb)
        slot = (m // nb) * nb + my_slot
        return remote(
            tok_ref, tok_all.at[m // nb, block_of(my_slot), :], tok_s.at[m], tok_r.at[slot],
            {"ep": to},
        )

    def tok_arrival(m):
        return remote(
            tok_ref, tok_all.at[m // nb, block_of(lax.rem(m, nb)), :], tok_s.at[m], tok_r.at[m],
            {"ep": lax.rem(me + 1, nep)},
        )

    def out_copy(m):
        to = group_at(my_group, m // nb) * nb + lax.rem(m, nb)
        return remote(
            out_send.at[m // nb, block_of(lax.rem(m, nb)), :], out_recv.at[me],
            out_s.at[m], out_r.at[me], {"ep": to},
        )

    def out_arrival(j):
        source = lax.rem(me + j, nep)
        return source, remote(
            out_send.at[0, block_of(0), :], out_recv.at[source],
            out_s.at[0], out_r.at[source], {"ep": source},
        )

    def ra_copy(k):
        return remote(ra.at[k], ra.at[k], ra_s.at[k], ra_r.at[k], {"tp": zl})

    def rb_copy(k):
        return remote(rb.at[k], rb.at[k], rb_s.at[k], rb_r.at[k], {"tp": zr})

    def ha_copy(k):
        return remote(ha.at[k], ha.at[k], ha_s.at[k], ha_r.at[k], {"tp": zr})

    def hb_copy(k):
        return remote(hb.at[k], hb.at[k], hb_s.at[k], hb_r.at[k], {"tp": zl})

    before = (
        lax.broadcasted_iota(jnp.int32, (span, span), 0)
        < lax.broadcasted_iota(jnp.int32, (span, span), 1)
    ).astype(bf16)

    def row_ids(d, lanes):
        r = lax.broadcasted_iota(jnp.int32, (full, lanes), 0)
        mine = 2 * r + d
        lent = 2 * full - 1 - d - 2 * (r - half)
        return jnp.where(r < half, mine, lent).astype(f32)
    sub_id = lax.broadcasted_iota(jnp.int32, (16, span), 0)

    def arrive(q):
        def one(i, carry):
            m = q * nb + i

            @pl.when(m != my_slot)
            def _():
                tok_arrival(m).wait_recv()

            return carry

        lax.fori_loop(0, nb, one, 0)

    def prepare(q):
        ids = meta_all[q, :top, :]
        fixed = meta_all[q, top:, :]
        chosen, wide = [], jnp.zeros((16, span), f32)
        for e in range(local):
            named = ids == me * local + e
            row = jnp.sum(named.astype(f32), axis=0, keepdims=True)
            weight = jnp.sum(jnp.where(named, fixed, 0), axis=0, keepdims=True)
            gate[q, e:e + 1, :] = weight.astype(f32) * (1.0 / 65536.0)
            wide = jnp.where(sub_id == e, row, wide)
            chosen.append(row)
        earlier = jnp.dot(wide.astype(bf16), before, preferred_element_type=f32)
        base = jnp.zeros((1, 1), f32)
        for e in range(local):
            place[q, e:e + 1, :] = jnp.where(
                chosen[e] > 0.5, base + earlier[e:e + 1, :], -1.0
            )
            base = base + jnp.sum(chosen[e], axis=1, keepdims=True)
            ends[q, e:e + 1, :] = jnp.broadcast_to(base, (1, LANES))

    prepare(0)
    pl.semaphore_wait(barrier, nep - 1 + sides)

    def send_tokens(m, carry):
        @pl.when(m != my_slot)
        def _():
            tok_copy(m).start()

        return carry

    lax.fori_loop(0, nep, send_tokens, 0)
    tok_all[0, block_of(my_slot), :] = tok_ref[...]

    def clear(j, carry):
        acc[j] = jnp.zeros(acc.shape[1:], acc.dtype)
        return carry

    lax.fori_loop(0, nq, clear, 0)

    def inside(u, part):
        fits = jnp.logical_and(u >= 0, u < 2 * chunks)
        return fits if part is None else jnp.logical_and(fits, lax.rem(u, 2) == part)

    def decode(k):
        c = lax.rem(k + late, chunks)
        return c // ng, lax.rem(c, ng)

    def spot(q, g):
        return lax.rem(q * ng + g + chunks - late, chunks)

    def lend_copy(k, d):
        i = d * chunks + k
        return remote(sp_out.at[i], sp_in.at[i], sp_s.at[i], sp_r.at[i], {"ep": partner})

    def back_copy(k, d, hidden):
        i = d * chunks + k
        return remote(
            hidden.at[k, pl.ds(low_row, spill), :], hs_in.at[i], hs_s.at[i], hs_r.at[i],
            {"ep": partner},
        )

    def product_stage(u, d):
        @pl.when(inside(u, 0))
        def _():
            k = u // 2
            q, g = decode(k)

            @pl.when(jnp.logical_or(k == 0, g == 0))
            def _():
                ids = row_ids(d, span)
                for e in range(local):
                    pick = ids == place[q, e:e + 1, :]
                    xbuf[d, e] = jnp.dot(
                        pick.astype(bf16), tok_all[q], preferred_element_type=f32
                    ).astype(bf16)

            total = jnp.dot(xbuf[d, 0], gu[g, 0], preferred_element_type=f32)
            for e in range(1, local):
                total += jnp.dot(xbuf[d, e], gu[g, e], preferred_element_type=f32)
            for p in range(2):
                own[d, lax.rem(k, 3), p] = total[:half, p * LANES:(p + 1) * LANES]
            if spill:
                sp_out[d * chunks + k] = total[half:]
                lend_copy(k, d).start()

    def chain_stage(u, d, buf, copy, has_source, is_last, hidden):
        @pl.when(inside(u, None))
        def _():
            k = u // 2
            p = lax.rem(u, 2)
            mine = own.at[d, lax.rem(k, 3), p]
            if spill:
                @pl.when(p == 0)
                def _():
                    lend_copy(k, d).wait_recv()
                    for i in range(2):
                        own[d, lax.rem(k, 3), i, low_row:, :] += sp_in[
                            d * chunks + k, :, i * LANES:(i + 1) * LANES
                        ]

            @pl.when(has_source)
            def _():
                copy(u).wait_recv()

            @pl.when(jnp.logical_and(has_source, jnp.logical_not(is_last)))
            def _():
                buf[u] = (mine[...] + buf[u].astype(f32)).astype(bf16)
                copy(u).start()

            @pl.when(jnp.logical_not(has_source))
            def _():
                buf[u] = mine[...].astype(bf16)
                copy(u).start()

            @pl.when(jnp.logical_and(is_last, p == 1))
            def _():
                v = own[d, lax.rem(k, 3), 0] + buf[u - 1].astype(f32)
                w = mine[...] + buf[u].astype(f32)
                hidden[k] = (v / (1.0 + jnp.exp(-v)) * w).astype(bf16)

    def hidden_stage(u, d, hidden, copy, has_source, is_last):
        @pl.when(inside(u, 1))
        def _():
            k = u // 2

            @pl.when(has_source)
            def _():
                copy(k).wait_recv()

            @pl.when(jnp.logical_not(is_last))
            def _():
                copy(k).start()

            if spill:
                back_copy(k, d, hidden).start()

    def down_stage(u, d, hidden):
        @pl.when(inside(u, 1))
        def _():
            k = u // 2
            if spill:
                back_copy(k, d, hidden).wait_recv()
            q, g = decode(k)
            home = (q == 0).astype(jnp.int32)

            @pl.when(lax.rem(g, pair) == pair - 1)
            def _():
                parts = [spot(q, g - pair + 1 + i) for i in range(pair)]
                units = jnp.concatenate([hidden[i] for i in parts], axis=1)
                if spill:
                    lent = jnp.concatenate([hs_in[d * chunks + i] for i in parts], axis=1)
                    units = jnp.concatenate([units, lent], axis=0)
                at = row_ids(d, LANES)
                start = jnp.zeros((1, LANES), f32)
                result = jnp.zeros((dw.shape[2], full), f32)
                for e in range(local):
                    end = ends[q, e:e + 1, :]
                    mine = jnp.logical_and(at >= start, at < end).astype(f32).astype(bf16)
                    start = end
                    result += lax.dot_general(
                        dw[g // pair, e], units * jnp.concatenate([mine] * pair, axis=1),
                        (((1,), (1,)), ((), ())), preferred_element_type=f32,
                    )
                first = jnp.logical_or(
                    k == pair - 1, jnp.logical_and(q > 0, g == pair - 1)
                )

                @pl.when(first)
                def _():
                    res[d, home] = result

                @pl.when(jnp.logical_not(first))
                def _():
                    res[d, home] += result

            @pl.when(complete(k))
            def _():
                ids = row_ids(d, span)
                top_part = jnp.zeros((full, span), f32)
                for e in range(local):
                    pick = ids == place[q, e:e + 1, :]
                    top_part = jnp.where(pick, gate[q, e:e + 1, :], top_part)
                coarse = top_part.astype(bf16)
                fine = (top_part - coarse.astype(f32)).astype(bf16)
                value = res[d, home]
                high = value.astype(bf16)
                low = (value - high.astype(f32)).astype(bf16)
                acc[q] += jnp.dot(
                    jnp.concatenate([high, high, low], axis=1),
                    jnp.concatenate([coarse, fine, coarse], axis=0),
                    preferred_element_type=f32,
                )

    def complete(k):
        q, g = decode(k)
        if late == 0:
            return g == ng - 1
        return jnp.logical_or(k == chunks - 1, jnp.logical_and(q > 0, g == ng - 1))

    turn = SKEW * (n - 1)
    from_right = SKEW * (n - 1 - z)
    from_left = SKEW * z
    lead = jnp.minimum(from_left, from_right)

    def step(t, carry):
        u_first = t - lead
        k_first = u_first // 2
        q_first, g_first = decode(k_first)

        @pl.when(jnp.logical_and(inside(u_first, 0), jnp.logical_and(q_first > 0, g_first == 0)))
        def _():
            prepare(q_first)
            arrive(q_first)

        @pl.when(jnp.logical_and(inside(u_first, 0), k_first < ng))
        def _():
            gate_copy(g_first).wait()
            up_copy(g_first).wait()

        @pl.when(t == LEAD + LATE + turn + lead + 2 * pair - 1)
        def _():
            for i in range(ng // pair):
                down_copy(i).wait()

        back = t - LEAD - turn - 1
        hidden_stage(back - from_left, 0, ha, ha_copy, z > 0, z == n - 1)
        hidden_stage(back - from_right, 1, hb, hb_copy, z < n - 1, z == 0)
        chain_stage(t - LEAD - from_right, 0, ra, ra_copy, z < n - 1, z == 0, ha)
        chain_stage(t - LEAD - from_left, 1, rb, rb_copy, z > 0, z == n - 1, hb)
        product_stage(t - from_right, 0)
        product_stage(t - from_left, 1)
        down_stage(back - LATE - from_left, 0, ha)
        down_stage(back - LATE - from_right, 1, hb)
        u_done = back - LATE - jnp.maximum(from_left, from_right)
        k_done = u_done // 2

        @pl.when(jnp.logical_and(inside(u_done, 1), complete(k_done)))
        def _():
            q, _ = decode(k_done)
            out_send[q] = acc[q].T.astype(bf16)

            def give(i, carry):
                m = q * nb + i

                @pl.when(m != my_slot)
                def _():
                    out_copy(m).start()

                return carry

            lax.fori_loop(0, nb, give, 0)

        return carry

    arrive(0)
    lax.fori_loop(0, 2 * chunks + 2 * turn + LEAD + LATE + 1, step, 0)

    def finish_chunk(k, carry):
        if spill:
            lend_copy(k, 0).wait_send()
            lend_copy(k, 1).wait_send()
            back_copy(k, 0, ha).wait_send()
            back_copy(k, 1, hb).wait_send()

        @pl.when(z > 0)
        def _():
            ra_copy(2 * k).wait_send()
            ra_copy(2 * k + 1).wait_send()
            hb_copy(k).wait_send()

        @pl.when(z < n - 1)
        def _():
            rb_copy(2 * k).wait_send()
            rb_copy(2 * k + 1).wait_send()
            ha_copy(k).wait_send()

        return carry

    lax.fori_loop(0, chunks, finish_chunk, 0)

    def finish_send(m, carry):
        @pl.when(m != my_slot)
        def _():
            tok_copy(m).wait_send()
            out_copy(m).wait_send()

        return carry

    lax.fori_loop(0, nep, finish_send, 0)
    total_out[...] = acc[0, :, block_of(my_slot)].T

    def finish_block(j, carry):
        source, copy = out_arrival(j)
        copy.wait_recv()
        total_out[...] += out_recv[source].astype(f32)
        return carry

    lax.fori_loop(1, nep, finish_block, 0)
    out_ref[...] = total_out[...].astype(bf16)


def count_call(nep, nq, local, limits, routing, gate_fixed):
    rows, top = routing.shape
    depth = 2 * top
    nb = nep // nq
    dma = pltpu.SemaphoreType.DMA
    vmem = pl.BlockSpec(memory_space=pltpu.VMEM)
    shape = (nq, depth, nb * rows)
    return pl.pallas_call(
        functools.partial(count_kernel, nep, nq, local, top, limits),
        out_shape=(
            jax.ShapeDtypeStruct(shape, jnp.int32), jax.ShapeDtypeStruct((1,), jnp.int32)
        ),
        in_specs=[vmem, vmem],
        out_specs=(vmem, pl.BlockSpec(memory_space=pltpu.SMEM)),
        scratch_shapes=[
            pltpu.VMEM((depth, rows), jnp.int32), pltpu.VMEM(shape, jnp.int32),
            dma((nep,)), dma((nep,)),
        ],
        compiler_params=pltpu.CompilerParams(collective_id=0, has_side_effects=True),
    )(routing.T, gate_fixed.T)


def layer_call(nep, n, nq, top, full, half, number, tokens, meta_all, gate_weight, up_weight, down_weight):
    local, share, width = gate_weight.shape
    rows = tokens.shape[0]
    nb = nep // nq
    ng = width // LANES
    chunks = nq * ng
    pair = 2 if ng % 2 == 0 else 1
    spill = max(full - half, 16)
    lent = 2 * chunks if half < full else 1
    bf16, f32 = jnp.bfloat16, jnp.float32
    dma = pltpu.SemaphoreType.DMA
    vmem = pl.BlockSpec(memory_space=pltpu.VMEM)
    hbm = pl.BlockSpec(memory_space=pl.ANY)
    return pl.pallas_call(
        functools.partial(layer_kernel, nep, n, local, top, nq, full, half),
        out_shape=jax.ShapeDtypeStruct((rows, share), bf16),
        in_specs=[vmem, vmem, hbm, hbm, hbm],
        out_specs=vmem,
        scratch_shapes=[
            pltpu.VMEM((ng, local, share, 2 * LANES), bf16),
            pltpu.VMEM((ng // pair, local, share, pair * LANES), bf16),
            pltpu.VMEM((nq, nb * rows, share), bf16),
            pltpu.VMEM((nq, 8, nb * rows), f32),
            pltpu.VMEM((nq, 8, nb * rows), f32),
            pltpu.VMEM((nq, 8, LANES), f32),
            pltpu.VMEM((2, local, full, share), bf16),
            pltpu.VMEM((2, 3, 2, half, LANES), f32),
            pltpu.VMEM((2, 2, share, full), f32),
            pltpu.VMEM((2 * chunks, half, LANES), bf16),
            pltpu.VMEM((2 * chunks, half, LANES), bf16),
            pltpu.VMEM((chunks, half, LANES), bf16),
            pltpu.VMEM((chunks, half, LANES), bf16),
            pltpu.VMEM((lent, spill, 2 * LANES), f32),
            pltpu.VMEM((lent, spill, 2 * LANES), f32),
            pltpu.VMEM((lent, spill, LANES), bf16),
            pltpu.VMEM((nq, share, nb * rows), f32),
            pltpu.VMEM((rows, share), f32),
            pltpu.VMEM((nq, nb * rows, share), bf16),
            pltpu.VMEM((nep, rows, share), bf16),
            dma((2, ng)), dma((ng // pair,)),
            dma((nep,)), dma((nep,)),
            dma((2 * chunks,)), dma((2 * chunks,)), dma((2 * chunks,)), dma((2 * chunks,)),
            dma((chunks,)), dma((chunks,)), dma((chunks,)), dma((chunks,)),
            dma((lent,)), dma((lent,)), dma((lent,)), dma((lent,)),
            dma((nep,)), dma((nep,)),
        ],
        compiler_params=pltpu.CompilerParams(
            collective_id=number, has_side_effects=True, vmem_limit_bytes=60 * 1024 * 1024
        ),
    )(tokens, meta_all, gate_weight, up_weight, down_weight)


def on_device(nep, n, tokens, routing, gate_fixed, gate_weight, up_weight, down_weight):
    local = gate_weight.shape[0]
    rows, top = routing.shape
    cap = max(2, rows * top * 2 // (local * nep))
    nq = next(c for c in (GROUPS, 2, 1) if nep % c == 0)
    full = nep // nq * local * cap // 2
    halves = [h for h in (full * s // 32 for s in SIZES) if h % 8 == 0] + [full]
    meta_all, size = count_call(
        nep, nq, local, [4 * h for h in halves[:-1]], routing, gate_fixed
    )
    calls = [
        functools.partial(layer_call, nep, n, nq, top, full, h, i + 1)
        for i, h in enumerate(halves)
    ]
    return lax.switch(
        size[0], calls, tokens, meta_all, gate_weight, up_weight, down_weight
    )


def solution(mesh):
    in_specs = (
        P("ep", "tp"),
        P("ep", None),
        P("ep", None),
        P("ep", "tp", None),
        P("ep", "tp", None),
        P("ep", "tp", None),
    )
    body = functools.partial(on_device, mesh.shape["ep"], mesh.shape["tp"])
    return jax.shard_map(
        body, mesh=mesh, in_specs=in_specs, out_specs=P("ep", "tp"), check_vma=False
    )
```
